8 devices in a mesh: dp: 2 (over z, y), tp: 4 (over x, core).
Axes of the slice: x: 2, y: 2, z: 1, core: 2. Of those that a mesh axis runs over, the one named last changes fastest.
Arguments:
- hidden_in: bfloat16 [512, 1024], P('dp'), parts along dimension 0
- k_cache: bfloat16 [512, 256, 8, 64], P('dp', None, 'tp'), parts along dimension 0
- v_cache: bfloat16 [512, 256, 8, 64], P('dp', None, 'tp'), parts along dimension 0
- seq_lens: int32 [512], P('dp'), parts along dimension 0
- chosen_experts: int32 [512, 8], P('dp'), parts along dimension 0
- g_attn: bfloat16 [1024], replicated
- w_q: bfloat16 [1024, 1024], P(None, 'tp')
- w_k: bfloat16 [1024, 512], P(None, 'tp')
- w_v: bfloat16 [1024, 512], P(None, 'tp')
- w_o: bfloat16 [1024, 1024], P('tp')
- g_moe: bfloat16 [1024], replicated
- w_router: bfloat16 [1024, 32], replicated
- w_gate: bfloat16 [32, 1024, 512], P(None, None, 'tp')
- w_up: bfloat16 [32, 1024, 512], P(None, None, 'tp')
- w_down: bfloat16 [32, 512, 1024], P(None, 'tp')
Outputs:
- output 1: bfloat16 [512, 1024], P('dp'), parts along dimension 0
- output 2: bfloat16 [512, 256, 8, 64], P('dp', None, 'tp'), parts along dimension 0
- output 3: bfloat16 [512, 256, 8, 64], P('dp', None, 'tp'), parts along dimension 0
There are 2 independent parts. The reference program is written for one: setup_inputs(seed, part) draws one part's arguments, and reference() takes and returns one part's arrays. A program takes and returns all parts, laid end to end along the dimension named above; an argument that names none is the same for every part.
All inputs are finite; a program needn't handle non-finite values.
Results may differ from the reference program's by a relative error of at most 0.00751233.
Values are sent between devices in bfloat16 or wider.
A program may use at most 1 GiB of HBM per device.

```python
import math
import jax
import jax.numpy as jnp
from jax import lax

BATCH_SEQS = 256
CACHE_LEN = 256
D_MODEL = 1024
Q_HEADS = 16
KV_HEADS = 8
HEAD_DIM = 64
FFN_DIM = 512
EXPERTS = 32
TOP_K = 8


def draw_layout(len_key, pick_key):
    seq_lens = jax.random.randint(len_key, (BATCH_SEQS,), 1, CACHE_LEN, dtype=jnp.int32)
    seq_lens = seq_lens.at[0].set(CACHE_LEN - 1)
    expert_ids = jnp.arange(EXPERTS, dtype=jnp.int32)
    hot_bonus = jnp.where(expert_ids < max(1, EXPERTS // 8), 2 * EXPERTS, 0)
    end_bonus = jnp.where((expert_ids == 0) | (expert_ids == EXPERTS - 1), 16 * EXPERTS, 0)
    first_row = (jnp.arange(BATCH_SEQS) == 0)[:, None]
    scores = jax.random.randint(pick_key, (BATCH_SEQS, EXPERTS), 0, 4 * EXPERTS, dtype=jnp.int32)
    scores = scores + hot_bonus[None, :] + jnp.where(first_row, end_bonus[None, :], 0)
    _, chosen_ids = lax.top_k(scores * EXPERTS + expert_ids[None, :], TOP_K)
    return seq_lens, chosen_ids.astype(jnp.int32)


def normal_weight(rng_key, out_shape, fan_in, factor):
    return (factor * fan_in ** -0.5 * jax.random.normal(rng_key, out_shape, jnp.float32)).astype(jnp.bfloat16)


def setup_inputs(seed: int = 0, part: int = 0) -> dict:
    part_keys = jax.random.split(jax.random.fold_in(jax.random.key(seed), part), 5)
    shared = jax.random.split(jax.random.key(seed + 1), 12)
    q_width = Q_HEADS * HEAD_DIM
    kv_width = KV_HEADS * HEAD_DIM
    key_scale = math.sqrt(0.75 * math.log(CACHE_LEN))
    cache_shape = (BATCH_SEQS, CACHE_LEN, KV_HEADS, HEAD_DIM)
    seq_lens, chosen_experts = draw_layout(part_keys[3], part_keys[4])
    return {
        "hidden_in": jax.random.normal(part_keys[0], (BATCH_SEQS, D_MODEL), jnp.float32).astype(jnp.bfloat16),
        "k_cache": (key_scale * jax.random.normal(part_keys[1], cache_shape, jnp.float32)).astype(jnp.bfloat16),
        "v_cache": jax.random.normal(part_keys[2], cache_shape, jnp.float32).astype(jnp.bfloat16),
        "seq_lens": seq_lens,
        "chosen_experts": chosen_experts,
        "g_attn": jax.random.uniform(shared[0], (D_MODEL,), jnp.float32, 0.5, 1.5).astype(jnp.bfloat16),
        "w_q": normal_weight(shared[1], (D_MODEL, q_width), D_MODEL, 1.0),
        "w_k": normal_weight(shared[2], (D_MODEL, kv_width), D_MODEL, 1.0),
        "w_v": normal_weight(shared[3], (D_MODEL, kv_width), D_MODEL, 1.0),
        "w_o": normal_weight(shared[4], (q_width, D_MODEL), q_width, 2.0),
        "g_moe": jax.random.uniform(shared[5], (D_MODEL,), jnp.float32, 0.5, 1.5).astype(jnp.bfloat16),
        "w_router": normal_weight(shared[6], (D_MODEL, EXPERTS), D_MODEL, 1.0),
        "w_gate": normal_weight(shared[7], (EXPERTS, D_MODEL, FFN_DIM), D_MODEL, 1.0),
        "w_up": normal_weight(shared[8], (EXPERTS, D_MODEL, FFN_DIM), D_MODEL, 1.0),
        "w_down": normal_weight(shared[9], (EXPERTS, FFN_DIM, D_MODEL), FFN_DIM, 2.0 * math.sqrt(TOP_K)),
    }


def rms_norm(vector, gain_w):
    vector32 = vector.astype(jnp.float32)
    norm_scale = lax.rsqrt(jnp.mean(vector32 * vector32, axis=-1, keepdims=True) + 1e-5)
    return (vector32 * norm_scale * gain_w.astype(jnp.float32)).astype(jnp.bfloat16)


def rope_rotate(vector, cos_t, sin_t):
    half_dim = vector.shape[-1] // 2
    lead_half = vector[..., :half_dim]
    tail_half = vector[..., half_dim:]
    return jnp.concatenate([lead_half * cos_t - tail_half * sin_t, tail_half * cos_t + lead_half * sin_t], axis=-1)


def attend_one(operands):
    q_seq, k_seq, v_seq, seq_len = operands
    scores = jnp.einsum("kgd,skd->kgs", q_seq.astype(jnp.float32), k_seq.astype(jnp.float32)) * HEAD_DIM ** -0.5
    in_range = (jnp.arange(CACHE_LEN) <= seq_len)[None, None, :]
    attn_weights = jax.nn.softmax(jnp.where(in_range, scores, -1e30), axis=-1).astype(jnp.bfloat16)
    return jnp.einsum("kgs,skd->kgd", attn_weights.astype(jnp.float32), v_seq.astype(jnp.float32)).astype(jnp.bfloat16)


def reference(hidden_in, k_cache, v_cache, seq_lens, chosen_experts, g_attn, w_q, w_k, w_v, w_o, g_moe, w_router, w_gate, w_up, w_down):
    q_group = Q_HEADS // KV_HEADS
    h_attn = rms_norm(hidden_in, g_attn)
    q_lin = jnp.dot(h_attn, w_q, preferred_element_type=jnp.float32).reshape(BATCH_SEQS, KV_HEADS, q_group, HEAD_DIM)
    k_lin = jnp.dot(h_attn, w_k, preferred_element_type=jnp.float32).reshape(BATCH_SEQS, KV_HEADS, HEAD_DIM)
    v_new = jnp.dot(h_attn, w_v, preferred_element_type=jnp.float32).reshape(BATCH_SEQS, KV_HEADS, HEAD_DIM).astype(jnp.bfloat16)
    inv_freq = 1000000.0 ** (-jnp.arange(0, HEAD_DIM, 2, dtype=jnp.float32) / HEAD_DIM)
    angles = seq_lens.astype(jnp.float32)[:, None] * inv_freq[None, :]
    cos_t = jnp.cos(angles)[:, None, :]
    sin_t = jnp.sin(angles)[:, None, :]
    q_rot = rope_rotate(q_lin, cos_t[:, :, None, :], sin_t[:, :, None, :]).astype(jnp.bfloat16)
    k_new = rope_rotate(k_lin, cos_t, sin_t).astype(jnp.bfloat16)
    new_slot = (jnp.arange(CACHE_LEN)[None, :] == seq_lens[:, None])[:, :, None, None]
    k_next = jnp.where(new_slot, k_new[:, None, :, :], k_cache)
    v_next = jnp.where(new_slot, v_new[:, None, :, :], v_cache)
    heads_out = lax.map(attend_one, (q_rot, k_next, v_next, seq_lens))
    attn_sum = jnp.dot(heads_out.reshape(BATCH_SEQS, Q_HEADS * HEAD_DIM), w_o, preferred_element_type=jnp.float32)
    hidden_mid = (hidden_in.astype(jnp.float32) + attn_sum).astype(jnp.bfloat16)
    h_moe = rms_norm(hidden_mid, g_moe)
    logits = jnp.dot(h_moe, w_router, preferred_element_type=jnp.float32)
    pick_mask = (chosen_experts[:, :, None] == jnp.arange(EXPERTS)[None, None, :]).astype(jnp.float32)
    gate_probs = jax.nn.softmax(jnp.sum(pick_mask * logits[:, None, :], axis=-1), axis=-1)
    gate_mat = jnp.sum(gate_probs[:, :, None] * pick_mask, axis=1)

    def expert_step(running, operands):
        gate_w, up_w, down_w, gate_col = operands
        up_gate = jnp.dot(h_moe, gate_w, preferred_element_type=jnp.float32)
        up_lin = jnp.dot(h_moe, up_w, preferred_element_type=jnp.float32)
        inner_act = (gate_col[:, None] * jax.nn.silu(up_gate) * up_lin).astype(jnp.bfloat16)
        return running + jnp.dot(inner_act, down_w, preferred_element_type=jnp.float32), None

    moe_sum, _ = lax.scan(expert_step, jnp.zeros((BATCH_SEQS, D_MODEL), jnp.float32), (w_gate, w_up, w_down, gate_mat.T))
    hidden_out = (hidden_mid.astype(jnp.float32) + moe_sum).astype(jnp.bfloat16)
    return (hidden_out, k_next, v_next)
```

```python
import jax
import jax.numpy as jnp
import numpy as np
from jax import lax
from jax.experimental import pallas as pl
from jax.experimental.pallas import tpu as pltpu
from jax.sharding import PartitionSpec as P

EPSILON = 1e-5
ROPE_THETA = 1000000.0
MASK_FILL = -1e30
BLOCK = 16
SLOTS = 8
AHEAD = 4
GROUP = 4


def normed(vector32, gain32):
    scale = lax.rsqrt(jnp.mean(vector32 * vector32, axis=-1, keepdims=True) + EPSILON)
    return (vector32 * scale * gain32).astype(jnp.bfloat16)


def attention_kernel(seq_s, seq_v, freq, gain, hidden, w_q, w_k, w_v, k_in, v_in, o_out, k_out, v_out,
                     hid, wqkv, kv_col, q_rows, o_rows, kbuf, vbuf, w_sem, k_rd, v_rd, k_wr, v_wr):
    rows, width, slots = k_in.shape
    heads_w = w_q.shape[1]
    half = width // 4
    steps = rows // BLOCK

    def read(i, slot):
        src = pl.ds(i * BLOCK, BLOCK)
        return (pltpu.make_async_copy(k_in.at[src], kbuf.at[slot], k_rd.at[slot]),
                pltpu.make_async_copy(v_in.at[src], vbuf.at[slot], v_rd.at[slot]))

    def write(i, slot):
        dst = pl.ds(i * BLOCK, BLOCK)
        return (pltpu.make_async_copy(kbuf.at[slot], k_out.at[dst], k_wr.at[slot]),
                pltpu.make_async_copy(vbuf.at[slot], v_out.at[dst], v_wr.at[slot]))

    loads = [pltpu.make_async_copy(hidden, hid, w_sem.at[0]),
             pltpu.make_async_copy(w_q, wqkv.at[:, 0:heads_w], w_sem.at[1]),
             pltpu.make_async_copy(w_k, wqkv.at[:, heads_w:heads_w + width], w_sem.at[2]),
             pltpu.make_async_copy(w_v, wqkv.at[:, heads_w + width:], w_sem.at[3])]
    for copy in loads:
        copy.start()
    for i in range(SLOTS):
        for copy in read(i, i):
            copy.start()
    angles = freq[...] * seq_v[...].astype(jnp.float32)
    cos_t, sin_t = jnp.cos(angles), jnp.sin(angles)
    for copy in loads:
        copy.wait()
    h = normed(hid[...].astype(jnp.float32), gain[...].astype(jnp.float32))
    qkv_t = jnp.dot(h, wqkv[...], preferred_element_type=jnp.float32).T

    def rotated(at):
        a, c = qkv_t[at:at + half], qkv_t[at + half:at + 2 * half]
        return [a * cos_t - c * sin_t, c * cos_t + a * sin_t]

    k_t = jnp.concatenate(rotated(heads_w) + rotated(heads_w + 2 * half), axis=0)
    v_t = qkv_t[heads_w + width:]
    for part in range(rows // 128):
        lanes = slice(part * 128, part * 128 + 128)
        kv_col[part, 0:width] = k_t[:, lanes].astype(jnp.bfloat16)
        kv_col[part, width:] = v_t[:, lanes].astype(jnp.bfloat16)
    lane = lax.broadcasted_iota(jnp.int32, (rows, width), 1)
    for g in range(2):
        q_g = jnp.concatenate(rotated(g * 2 * half) + rotated((2 + g) * 2 * half), axis=0).T
        q_g = q_g.astype(jnp.bfloat16).astype(jnp.float32) * 0.125
        for kv in range(2):
            keep = (lane < 2 * half) if kv == 0 else (lane >= 2 * half)
            q_rows[pl.ds(kv * 2 + g, rows, stride=8), :] = jnp.where(keep, q_g, 0.0)
    for r in range(4, 8):
        q_rows[pl.ds(r, rows, stride=8), :] = jnp.zeros((rows, width), jnp.float32)

    slot_id = lax.broadcasted_iota(jnp.int32, (8, slots), 1)
    slot_bf = lax.broadcasted_iota(jnp.int32, (width, slots), 1).astype(jnp.float32).astype(jnp.bfloat16)

    row_id = lax.broadcasted_iota(jnp.int32, (128, 256), 0) - lax.div(lax.broadcasted_iota(jnp.int32, (128, 256), 1), 128)
    row_bf = row_id.astype(jnp.float32).astype(jnp.bfloat16)

    def step(i, carry):
        slot = lax.rem(i, SLOTS)
        for copy in read(i, slot):
            copy.wait()
        per = 128 // BLOCK
        columns = kv_col[lax.div(i, per)]
        first_row = lax.rem(i, per) * BLOCK
        cols = []
        for j in range(0, BLOCK, 2):
            pick = (row_bf == (first_row + j).astype(jnp.float32).astype(jnp.bfloat16))
            pick = jnp.where(pick, jnp.ones((), jnp.bfloat16), jnp.zeros((), jnp.bfloat16))
            both = jnp.dot(columns, pick, preferred_element_type=jnp.float32).astype(jnp.bfloat16)
            cols += [both[:, 0:128], both[:, 128:256]]
        places = [seq_s[i * BLOCK + j] for j in range(BLOCK)]

        def updated(buf, j, at):
            col = jnp.concatenate([cols[j][at:at + width]] * (slots // 128), axis=1)
            here = slot_bf == places[j].astype(jnp.float32).astype(jnp.bfloat16)
            new = jnp.where(here, col, buf[slot, j])
            buf[slot, j] = new
            return new

        scores = []
        for j in range(BLOCK):
            q = q_rows[pl.ds((i * BLOCK + j) * 8, 8), :].astype(jnp.bfloat16)
            s = jnp.dot(q, updated(kbuf, j, 0), preferred_element_type=jnp.float32)
            scores.append(jnp.where(slot_id <= places[j], s, MASK_FILL))
        for j in range(BLOCK):
            s = scores[j]
            e = jnp.exp(s - jnp.max(s, axis=-1, keepdims=True))
            w = (e / jnp.sum(e, axis=-1, keepdims=True)).astype(jnp.bfloat16)
            o = lax.dot_general(w, updated(vbuf, j, width), (((1,), (1,)), ((), ())), preferred_element_type=jnp.float32)
            o_rows[pl.ds(j * 8, 8), :] = o
        for copy in write(i, slot):
            copy.start()
        low = lax.broadcasted_iota(jnp.int32, (BLOCK, width), 1) < 2 * half
        for kv in range(2):
            first = o_rows[pl.ds(2 * kv, BLOCK, stride=8), :]
            second = o_rows[pl.ds(2 * kv + 1, BLOCK, stride=8), :]
            if kv == 0:
                second = pltpu.roll(second, 2 * half, axis=1)
            else:
                first = pltpu.roll(first, 2 * half, axis=1)
            o_out[pl.ds(i * BLOCK, BLOCK), kv * width:(kv + 1) * width] = jnp.where(low, first, second).astype(jnp.bfloat16)

        @pl.when(jnp.logical_and(i >= AHEAD, i < steps - SLOTS + AHEAD))
        def _():
            old = lax.rem(i + SLOTS - AHEAD, SLOTS)
            for copy in write(i - AHEAD, old):
                copy.wait()
            for copy in read(i + SLOTS - AHEAD, old):
                copy.start()
        return carry

    lax.fori_loop(0, steps, step, 0)
    for i in range(steps - SLOTS, steps):
        for copy in write(i, i % SLOTS):
            copy.wait()


def attention_call(hidden_in, k_t, v_t, seq_lens, g_attn, w_q, w_k, w_v):
    rows, width, slots = k_t.shape
    any_spec = pl.BlockSpec(memory_space=pltpu.HBM)
    vmem = pl.BlockSpec(memory_space=pltpu.VMEM)
    freq = (ROPE_THETA ** (-np.arange(0, 64, 2) / 64)).astype(np.float32)
    cache = jax.ShapeDtypeStruct(k_t.shape, k_t.dtype)
    dma = pltpu.SemaphoreType.DMA
    return pl.pallas_call(
        attention_kernel,
        out_shape=(jax.ShapeDtypeStruct((rows, w_q.shape[1]), jnp.bfloat16), cache, cache),
        in_specs=[pl.BlockSpec(memory_space=pltpu.SMEM), vmem, vmem, vmem] + [any_spec] * 6,
        out_specs=(vmem, any_spec, any_spec),
        scratch_shapes=[
            pltpu.VMEM(hidden_in.shape, jnp.bfloat16),
            pltpu.VMEM((hidden_in.shape[1], w_q.shape[1] + 2 * width), jnp.bfloat16),
            pltpu.VMEM((rows // 128, 2 * width, 128), jnp.bfloat16),
            pltpu.VMEM((rows * 8, width), jnp.float32),
            pltpu.VMEM((BLOCK * 8, width), jnp.float32),
            pltpu.VMEM((SLOTS, BLOCK, width, slots), jnp.bfloat16),
            pltpu.VMEM((SLOTS, BLOCK, width, slots), jnp.bfloat16),
            dma((4,)), dma((SLOTS,)), dma((SLOTS,)), dma((SLOTS,)), dma((SLOTS,)),
        ],
        compiler_params=pltpu.CompilerParams(vmem_limit_bytes=60 << 20),
        cost_estimate=pl.CostEstimate(flops=10**9, bytes_accessed=70 * 10**6, transcendentals=0),
        name="attention",
    )(seq_lens, seq_lens.reshape(1, rows), freq.reshape(32, 1), g_attn.reshape(1, -1), hidden_in, w_q, w_k, w_v, k_t, v_t)


def expert_kernel(o_in, chosen, gain, router, hidden, wo_own, wo_peer, w_gate, w_up, w_down, out,
                  hid, wo_full, o_full, w_in, w_dn, x1, h2_buf, gates, z, acc, from_pair, chip_sum, from_far,
                  ld_sem, wi_sem, wd_sem, wo_snd, wo_rcv, o_snd, o_rcv, a_snd, a_rcv, b_snd, b_rcv, c_snd, c_rcv):
    experts, dim, part = w_gate.shape
    rows = hid.shape[0]
    half = rows // 2
    quarter, eighth = half // 2, half // 4
    cols = dim // 2
    groups = w_in.shape[0] // GROUP
    me = lax.axis_index("tp")
    core, chip = lax.rem(me, 2), lax.div(me, 2)
    pair, far = me + 1 - 2 * core, me + 2 - 4 * chip
    pair_far = far + 1 - 2 * core

    def remote(src, dst, send, recv, to):
        return pltpu.make_async_remote_copy(src_ref=src, dst_ref=dst, send_sem=send, recv_sem=recv,
                                            device_id={"tp": to}, device_id_type=pl.DeviceIdType.MESH)

    def load_in(g):
        sl = pl.ds(g * GROUP, GROUP)
        return (pltpu.make_async_copy(w_gate.at[sl], w_in.at[sl, :, 0:part], wi_sem.at[0, g]),
                pltpu.make_async_copy(w_up.at[sl], w_in.at[sl, :, part:2 * part], wi_sem.at[1, g]))

    def load_down(g):
        sl = pl.ds(g * (w_dn.shape[0] // 4), w_dn.shape[0] // 4)
        return pltpu.make_async_copy(w_down.at[sl], w_dn.at[sl], wd_sem.at[g])

    loads = [pltpu.make_async_copy(hidden, hid, ld_sem.at[0]),
             pltpu.make_async_copy(wo_own, wo_full.at[me], ld_sem.at[1]),
             pltpu.make_async_copy(wo_peer, wo_full.at[far], ld_sem.at[2])]
    for copy in loads:
        copy.start()
    for g in range(groups):
        for copy in load_in(g):
            copy.start()
    for g in range(4):
        load_down(g).start()

    barrier = pltpu.get_barrier_semaphore()
    for peer in (pair, far):
        pl.semaphore_signal(barrier, inc=1, device_id={"tp": peer}, device_id_type=pl.DeviceIdType.MESH)
    pl.semaphore_wait(barrier, 2)

    def o_block(owner, h, kind, to):
        src = o_in.at[pl.ds(h * half, half)] if kind < 2 else o_full.at[owner, pl.ds(h * half, half)]
        return remote(src, o_full.at[owner, pl.ds(h * half, half)], o_snd.at[kind, h], o_rcv.at[kind, h], to)

    sends = []

    def go(copy):
        copy.start()
        sends.append(copy)

    for h in range(2):
        go(o_block(me, h, 0, far))
    for h in range(2):
        go(o_block(me, h, 1, pair))
    go(remote(wo_own, wo_full.at[me], wo_snd.at[0], wo_rcv.at[0], pair))
    go(remote(wo_peer, wo_full.at[far], wo_snd.at[1], wo_rcv.at[1], pair))
    o_full[me] = o_in[...]

    def relay_o(h):
        o_block(far, h, 0, far).wait_recv()
        go(o_block(far, h, 2, pair))

    def mid(h):
        o_block(pair, h, 1, pair).wait_recv()
        o_block(pair_far, h, 2, pair).wait_recv()
        at = pl.ds(h * half, half)
        total = hid[at, :].astype(jnp.float32)
        for r in range(4):
            total = total + jnp.dot(o_full[r, at, :], wo_full[r], preferred_element_type=jnp.float32)
        x1[at, :] = total.astype(jnp.bfloat16)

    def routed(h):
        at = pl.ds(h * half, half)
        h2 = normed(x1[at, :].astype(jnp.float32), gain[...].astype(jnp.float32))
        logits = lax.dot_general(router[...], h2, (((1,), (1,)), ((), ())), preferred_element_type=jnp.float32)
        expert_id = lax.broadcasted_iota(jnp.int32, logits.shape, 0)
        picks = chosen[:, h * half:(h + 1) * half]
        hit = expert_id == picks[0:1]
        for k in range(1, picks.shape[0]):
            hit = jnp.logical_or(hit, expert_id == picks[k:k + 1])
        shown = jnp.where(hit, logits, MASK_FILL)
        e = jnp.where(hit, jnp.exp(shown - jnp.max(shown, axis=0, keepdims=True)), 0.0)
        g = e / jnp.sum(e, axis=0, keepdims=True)
        gates[h] = jnp.concatenate([g, jnp.zeros((128 - experts, half), jnp.float32)], axis=0).T
        return h2

    lane = lax.broadcasted_iota(jnp.int32, (half, 128), 1)

    def inner(h, h2_ref, lo, hi):
        def group(g, carry):
            if h == 0:
                for copy in load_in(g):
                    copy.wait()
            for k in range(GROUP):
                e = g * GROUP + k
                both = jnp.dot(h2_ref[...], w_in[e], preferred_element_type=jnp.float32)
                gate, up = both[:, :part], both[:, part:]
                weight = jnp.sum(jnp.where(lane == e, gates[h], 0.0), axis=1, keepdims=True)
                act = weight * (gate / (1.0 + jnp.exp(-gate))) * up
                z[:, pl.ds(pl.multiple_of(e * part, part), part)] = act.astype(jnp.bfloat16)
            return carry
        lax.fori_loop(lo, hi, group, 0)

    def down(h, c):
        acc[h, c] = jnp.dot(z[...], w_dn[:, c * cols:(c + 1) * cols], preferred_element_type=jnp.float32)

    def pair_copy(h, c):
        return remote(acc.at[h, c, pl.ds((1 - core) * quarter, quarter)], from_pair.at[h, c], a_snd.at[h, c], a_rcv.at[h, c], pair)

    def far_copy(h, c):
        return remote(chip_sum.at[h, c, pl.ds((1 - chip) * eighth, eighth)], from_far.at[h, c], b_snd.at[h, c], b_rcv.at[h, c], far)

    def out_copy(h, c, kind, block_core, block_chip, to):
        at = out.at[pl.ds(h * half + block_core * quarter + block_chip * eighth, eighth), c * cols:(c + 1) * cols]
        return remote(at, at, c_snd.at[kind, h, c], c_rcv.at[kind, h, c], to)

    def stage_b(h, c):
        pair_copy(h, c).wait_recv()
        chip_sum[h, c] = acc[h, c, pl.ds(core * quarter, quarter)] + from_pair[h, c]
        go(far_copy(h, c))

    def stage_c(h, c):
        far_copy(h, c).wait_recv()
        at = pl.ds(h * half + core * quarter + chip * eighth, eighth)
        cut = slice(c * cols, (c + 1) * cols)
        total = chip_sum[h, c, pl.ds(chip * eighth, eighth)] + from_far[h, c]
        out[at, cut] = (x1[at, cut].astype(jnp.float32) + total).astype(jnp.bfloat16)
        go(out_copy(h, c, 0, core, chip, far))
        go(out_copy(h, c, 1, core, chip, pair))

    def stage_d(h, c):
        out_copy(h, c, 0, core, 1 - chip, far).wait_recv()
        go(out_copy(h, c, 2, core, 1 - chip, pair))

    def stage_e(h, c):
        out_copy(h, c, 1, 1 - core, chip, pair).wait_recv()
        out_copy(h, c, 2, 1 - core, 1 - chip, pair).wait_recv()

    relay_o(0)
    for copy in loads:
        copy.wait()
    remote(wo_own, wo_full.at[pair], wo_snd.at[0], wo_rcv.at[0], pair).wait_recv()
    remote(wo_peer, wo_full.at[pair_far], wo_snd.at[1], wo_rcv.at[1], pair).wait_recv()
    mid(0)
    relay_o(1)

    def with_h2(h, h2_ref):
        h2_ref[...] = routed(h)

    def first_half(h2_ref):
        with_h2(0, h2_ref)
        inner(0, h2_ref, 0, groups)
        for g in range(4):
            load_down(g).wait()
        for c in range(2):
            down(0, c)
            go(pair_copy(0, c))
        mid(1)
        with_h2(1, h2_ref)
        for c in range(2):
            stage_b(0, c)
        inner(1, h2_ref, 0, groups // 2)
        for c in range(2):
            stage_c(0, c)
        inner(1, h2_ref, groups // 2, groups)
        for c in range(2):
            stage_d(0, c)
        for c in range(2):
            down(1, c)
            go(pair_copy(1, c))

    first_half(h2_buf)
    for stage in (stage_b, stage_c, stage_d):
        for c in range(2):
            stage(1, c)
    for h in range(2):
        for c in range(2):
            stage_e(h, c)
    for copy in sends:
        copy.wait_send()


def expert_call(o, hidden_in, chosen_t, g_moe, router_t, w_o, wo_peer, w_gate, w_up, w_down):
    rows, dim = hidden_in.shape
    experts, _, part = w_gate.shape
    half, cols = rows // 2, dim // 2
    any_spec = pl.BlockSpec(memory_space=pltpu.HBM)
    vmem = pl.BlockSpec(memory_space=pltpu.VMEM)
    dma = pltpu.SemaphoreType.DMA
    bf, f32 = jnp.bfloat16, jnp.float32
    return pl.pallas_call(
        expert_kernel,
        out_shape=jax.ShapeDtypeStruct((rows, dim), bf),
        in_specs=[vmem] * 4 + [any_spec] * 6,
        out_specs=vmem,
        scratch_shapes=[
            pltpu.VMEM((rows, dim), bf),
            pltpu.VMEM((4,) + w_o.shape, bf),
            pltpu.VMEM((4,) + o.shape, bf),
            pltpu.VMEM((experts, dim, 2 * part), bf),
            pltpu.VMEM((experts * part, dim), bf),
            pltpu.VMEM((rows, dim), bf),
            pltpu.VMEM((half, dim), bf),
            pltpu.VMEM((2, half, 128), f32),
            pltpu.VMEM((half, experts * part), bf),
            pltpu.VMEM((2, 2, half, cols), f32),
            pltpu.VMEM((2, 2, half // 2, cols), f32),
            pltpu.VMEM((2, 2, half // 2, cols), f32),
            pltpu.VMEM((2, 2, half // 4, cols), f32),
            dma((3,)), dma((2, experts // GROUP)), dma((4,)), dma((2,)), dma((2,)), dma((3, 2)), dma((3, 2)),
            dma((2, 2)), dma((2, 2)), dma((2, 2)), dma((2, 2)), dma((3, 2, 2)), dma((3, 2, 2)),
        ],
        compiler_params=pltpu.CompilerParams(collective_id=0, has_side_effects=True, vmem_limit_bytes=60 << 20),
        cost_estimate=pl.CostEstimate(flops=7 * 10**9, bytes_accessed=28 * 10**6, transcendentals=0),
        name="experts",
    )(o, chosen_t, g_moe.reshape(1, -1), router_t, hidden_in, w_o, wo_peer, w_gate, w_up, w_down.reshape(experts * part, dim))


def solution(mesh):
    cache_spec = P("dp", None, "tp", None)
    in_specs = (P("dp", None), cache_spec, cache_spec, P("dp"), P("dp", None), P(None), P(None, "tp"), P(None, "tp"), P(None, "tp"), P("tp", None), P(None), P(None, None), P(None, None, "tp"), P(None, None, "tp"), P(None, "tp", None))
    out_specs = (P("dp", None), cache_spec, cache_spec)

    def layer_shard(hidden_in, k_cache, v_cache, seq_lens, chosen_experts, g_attn, w_q, w_k, w_v, w_o, g_moe, w_router, w_gate, w_up, w_down):
        rows, slots, kvh, hd = k_cache.shape
        as_t = lambda c: c.transpose(0, 2, 3, 1).reshape(rows, kvh * hd, slots)
        back = lambda c: c.reshape(rows, kvh, hd, slots).transpose(0, 3, 1, 2)
        wo_peer = lax.ppermute(w_o, "tp", [(0, 2), (1, 3), (2, 0), (3, 1)])
        o, k_n, v_n = attention_call(hidden_in, as_t(k_cache), as_t(v_cache), seq_lens, g_attn, w_q, w_k, w_v)
        hidden_out = expert_call(o, hidden_in, chosen_experts.T, g_moe, w_router.T, w_o, wo_peer, w_gate, w_up, w_down)
        return hidden_out, back(k_n), back(v_n)

    return jax.shard_map(layer_shard, mesh=mesh, in_specs=in_specs, out_specs=out_specs, check_vma=False)
```

```python
import math
import jax
import jax.numpy as jnp
from jax import lax
from jax.experimental import pallas as pl
from jax.experimental.pallas import tpu as pltpu
from jax.sharding import PartitionSpec as P

EPSILON = 1e-5
ROPE_THETA = 1000000.0
MASK_FILL = -1e30
BLOCK = 16
SLOTS = 8
AHEAD = 4
GROUP = 4
UNROLL = 8
PARTS = 2
CHUNKS = 2
DIRECT = 0


def pinned(array):
    return pltpu.with_memory_space_constraint(array, pltpu.HBM)


def normed(vector32, gain32):
    scale = lax.rsqrt(jnp.mean(vector32 * vector32, axis=-1, keepdims=True) + EPSILON)
    return (vector32 * scale * gain32).astype(jnp.bfloat16)


def attention_kernel(seq_lens, g_attn, hidden, w_q, w_k, w_v, k_in, v_in, o_out, k_out, v_out,
                     seq_s, seq_v, gain, hid, wqkv, kv_col, q_rows, o_rows, kbuf, vbuf, w_sem, k_rd, v_rd, k_wr, v_wr):
    rows, width, slots = k_in.shape
    heads_w = w_q.shape[1]
    half = width // 4
    steps = rows // BLOCK

    def read(i, slot):
        src = pl.ds(i * BLOCK, BLOCK)
        return (pltpu.make_async_copy(k_in.at[src], kbuf.at[slot], k_rd.at[slot]),
                pltpu.make_async_copy(v_in.at[src], vbuf.at[slot], v_rd.at[slot]))

    def write(i, slot):
        dst = pl.ds(i * BLOCK, BLOCK)
        return (pltpu.make_async_copy(kbuf.at[slot], k_out.at[dst], k_wr.at[slot]),
                pltpu.make_async_copy(vbuf.at[slot], v_out.at[dst], v_wr.at[slot]))

    loads = [pltpu.make_async_copy(hidden, hid, w_sem.at[0]),
             pltpu.make_async_copy(w_q, wqkv.at[:, 0:heads_w], w_sem.at[1]),
             pltpu.make_async_copy(w_k, wqkv.at[:, heads_w:heads_w + width], w_sem.at[2]),
             pltpu.make_async_copy(w_v, wqkv.at[:, heads_w + width:], w_sem.at[3]),
             pltpu.make_async_copy(seq_lens, seq_v, w_sem.at[4]),
             pltpu.make_async_copy(seq_lens, seq_s, w_sem.at[5]),
             pltpu.make_async_copy(g_attn, gain, w_sem.at[6])]
    for copy in loads:
        copy.start()
    for i in range(SLOTS):
        for copy in read(i, i):
            copy.start()
    loads[4].wait()
    place = lax.broadcasted_iota(jnp.int32, (half, rows), 0).astype(jnp.float32)
    angles = jnp.exp(place * (-math.log(ROPE_THETA) / half)) * seq_v[...].astype(jnp.float32)[None, :]
    cos_t, sin_t = jnp.cos(angles), jnp.sin(angles)
    for copy in loads[:4] + loads[5:]:
        copy.wait()
    h = normed(hid[...].astype(jnp.float32), gain[...].astype(jnp.float32))
    qkv_t = jnp.dot(h, wqkv[...], preferred_element_type=jnp.float32).T

    def rotated(at):
        a, c = qkv_t[at:at + half], qkv_t[at + half:at + 2 * half]
        return [a * cos_t - c * sin_t, c * cos_t + a * sin_t]

    k_t = jnp.concatenate(rotated(heads_w) + rotated(heads_w + 2 * half), axis=0)
    v_t = qkv_t[heads_w + width:]
    for part in range(rows // 128):
        lanes = slice(part * 128, part * 128 + 128)
        kv_col[part, 0:width] = k_t[:, lanes].astype(jnp.bfloat16)
        kv_col[part, width:] = v_t[:, lanes].astype(jnp.bfloat16)
    lane = lax.broadcasted_iota(jnp.int32, (rows, width), 1)
    for g in range(2):
        q_g = jnp.concatenate(rotated(g * 2 * half) + rotated((2 + g) * 2 * half), axis=0).T
        q_g = q_g.astype(jnp.bfloat16).astype(jnp.float32) * 0.125
        for kv in range(2):
            keep = (lane < 2 * half) if kv == 0 else (lane >= 2 * half)
            q_rows[pl.ds(kv * 2 + g, rows, stride=8), :] = jnp.where(keep, q_g, 0.0)
    for r in range(4, 8):
        q_rows[pl.ds(r, rows, stride=8), :] = jnp.zeros((rows, width), jnp.float32)

    slot_id = lax.broadcasted_iota(jnp.int32, (8, slots), 1)
    slot_bf = lax.broadcasted_iota(jnp.int32, (width, slots), 1).astype(jnp.float32).astype(jnp.bfloat16)

    row_id = lax.broadcasted_iota(jnp.int32, (128, 256), 0) - lax.div(lax.broadcasted_iota(jnp.int32, (128, 256), 1), 128)
    row_bf = row_id.astype(jnp.float32).astype(jnp.bfloat16)

    def step(i, carry):
        slot = lax.rem(i, SLOTS)
        for copy in read(i, slot):
            copy.wait()
        per = 128 // BLOCK
        columns = kv_col[lax.div(i, per)]
        first_row = lax.rem(i, per) * BLOCK
        cols = []
        for j in range(0, BLOCK, 2):
            pick = (row_bf == (first_row + j).astype(jnp.float32).astype(jnp.bfloat16))
            pick = jnp.where(pick, jnp.ones((), jnp.bfloat16), jnp.zeros((), jnp.bfloat16))
            both = jnp.dot(columns, pick, preferred_element_type=jnp.float32).astype(jnp.bfloat16)
            cols += [both[:, 0:128], both[:, 128:256]]
        places = [seq_s[i * BLOCK + j] for j in range(BLOCK)]

        def updated(buf, j, at):
            col = jnp.concatenate([cols[j][at:at + width]] * (slots // 128), axis=1)
            here = slot_bf == places[j].astype(jnp.float32).astype(jnp.bfloat16)
            new = jnp.where(here, col, buf[slot, j])
            buf[slot, j] = new
            return new

        scores = []
        for j in range(BLOCK):
            q = q_rows[pl.ds((i * BLOCK + j) * 8, 8), :].astype(jnp.bfloat16)
            s = jnp.dot(q, updated(kbuf, j, 0), preferred_element_type=jnp.float32)
            scores.append(jnp.where(slot_id <= places[j], s, MASK_FILL))
        for j in range(BLOCK):
            s = scores[j]
            e = jnp.exp(s - jnp.max(s, axis=-1, keepdims=True))
            w = (e / jnp.sum(e, axis=-1, keepdims=True)).astype(jnp.bfloat16)
            o = lax.dot_general(w, updated(vbuf, j, width), (((1,), (1,)), ((), ())), preferred_element_type=jnp.float32)
            o_rows[pl.ds(j * 8, 8), :] = o
        for copy in write(i, slot):
            copy.start()
        low = lax.broadcasted_iota(jnp.int32, (BLOCK, width), 1) < 2 * half
        for kv in range(2):
            first = o_rows[pl.ds(2 * kv, BLOCK, stride=8), :]
            second = o_rows[pl.ds(2 * kv + 1, BLOCK, stride=8), :]
            if kv == 0:
                second = pltpu.roll(second, 2 * half, axis=1)
            else:
                first = pltpu.roll(first, 2 * half, axis=1)
            o_out[pl.ds(i * BLOCK, BLOCK), kv * width:(kv + 1) * width] = jnp.where(low, first, second).astype(jnp.bfloat16)

        @pl.when(jnp.logical_and(i >= AHEAD, i < steps - SLOTS + AHEAD))
        def _():
            old = lax.rem(i + SLOTS - AHEAD, SLOTS)
            for copy in write(i - AHEAD, old):
                copy.wait()
            for copy in read(i + SLOTS - AHEAD, old):
                copy.start()
        return carry

    lax.fori_loop(0, steps, step, 0)
    for i in range(steps - SLOTS, steps):
        for copy in write(i, i % SLOTS):
            copy.wait()


def attention_call(hidden_in, k_t, v_t, seq_lens, g_attn, w_q, w_k, w_v):
    rows, width, slots = k_t.shape
    any_spec = pl.BlockSpec(memory_space=pltpu.HBM)
    vmem = pl.BlockSpec(memory_space=pltpu.VMEM)
    cache = jax.ShapeDtypeStruct(k_t.shape, k_t.dtype)
    dma = pltpu.SemaphoreType.DMA
    return pl.pallas_call(
        attention_kernel,
        out_shape=(jax.ShapeDtypeStruct((rows, w_q.shape[1]), jnp.bfloat16), cache, cache),
        in_specs=[any_spec] * 8,
        out_specs=(vmem, any_spec, any_spec),
        scratch_shapes=[
            pltpu.SMEM(seq_lens.shape, jnp.int32),
            pltpu.VMEM(seq_lens.shape, jnp.int32),
            pltpu.VMEM(g_attn.shape, jnp.bfloat16),
            pltpu.VMEM(hidden_in.shape, jnp.bfloat16),
            pltpu.VMEM((hidden_in.shape[1], w_q.shape[1] + 2 * width), jnp.bfloat16),
            pltpu.VMEM((rows // 128, 2 * width, 128), jnp.bfloat16),
            pltpu.VMEM((rows * 8, width), jnp.float32),
            pltpu.VMEM((BLOCK * 8, width), jnp.float32),
            pltpu.VMEM((SLOTS, BLOCK, width, slots), jnp.bfloat16),
            pltpu.VMEM((SLOTS, BLOCK, width, slots), jnp.bfloat16),
            dma((7,)), dma((SLOTS,)), dma((SLOTS,)), dma((SLOTS,)), dma((SLOTS,)),
        ],
        compiler_params=pltpu.CompilerParams(vmem_limit_bytes=26 << 20),
        cost_estimate=pl.CostEstimate(flops=10**9, bytes_accessed=70 * 10**6, transcendentals=0),
        name="attention",
    )(*(pinned(a) for a in (seq_lens, g_attn, hidden_in, w_q, w_k, w_v, k_t, v_t)))


def expert_kernel(o_in, chosen, gain, router, hid, wo_own, wo_peer, w_gate, w_up, w_down, out,
                  wo_pair, wo_pair_far, o_full, w_in, w_dn, x1, h2, gates, z, acc, from_pair, chip_sum, from_far,
                  wi_sem, wd_sem, wo_snd, wo_rcv, o_snd, o_rcv, a_snd, a_rcv, b_snd, b_rcv, c_snd, c_rcv):
    experts, dim, part = w_gate.shape
    rows = hid.shape[0]
    o_rows = rows // 2
    block = rows // PARTS
    cols = dim // CHUNKS
    groups = experts // GROUP
    me = lax.axis_index("tp")
    core, chip = lax.rem(me, 2), lax.div(me, 2)
    pair, far = me + 1 - 2 * core, me + 2 - 4 * chip
    pair_far = far + 1 - 2 * core

    def remote(src, dst, send, recv, to):
        return pltpu.make_async_remote_copy(src_ref=src, dst_ref=dst, send_sem=send, recv_sem=recv,
                                            device_id={"tp": to}, device_id_type=pl.DeviceIdType.MESH)

    def load_in(g):
        sl = pl.ds(g * GROUP, GROUP)
        return (pltpu.make_async_copy(w_gate.at[sl], w_in.at[sl, :, 0:part], wi_sem.at[0, g]),
                pltpu.make_async_copy(w_up.at[sl], w_in.at[sl, :, part:2 * part], wi_sem.at[1, g]))

    def load_down(g):
        sl = pl.ds(g * (w_dn.shape[0] // 4), w_dn.shape[0] // 4)
        return pltpu.make_async_copy(w_down.at[sl], w_dn.at[sl], wd_sem.at[g])

    barrier = pltpu.get_barrier_semaphore()
    for peer in (pair, far):
        pl.semaphore_signal(barrier, inc=1, device_id={"tp": peer}, device_id_type=pl.DeviceIdType.MESH)
    for g in range(groups):
        for copy in load_in(g):
            copy.start()
    for g in range(4):
        load_down(g).start()
    pl.semaphore_wait(barrier, 2)

    def o_block(owner, h, kind, to):
        at = pl.ds(h * o_rows, o_rows)
        src = o_in.at[at] if kind < 2 else o_full.at[owner, at]
        return remote(src, o_full.at[owner, at], o_snd.at[kind, h], o_rcv.at[kind, h], to)

    sends = []

    def go(copy):
        copy.start()
        sends.append(copy)

    wo_copies = [remote(wo_own, wo_pair, wo_snd.at[0], wo_rcv.at[0], pair),
                 remote(wo_peer, wo_pair_far, wo_snd.at[1], wo_rcv.at[1], pair)]
    for h in range(2):
        go(o_block(me, h, 0, far))
    for h in range(2):
        go(o_block(me, h, 1, pair))
    for copy in wo_copies:
        go(copy)

    def relay_o(h):
        o_block(far, h, 0, far).wait_recv()
        go(o_block(far, h, 2, pair))

    def mid(h):
        o_block(pair, h, 1, pair).wait_recv()
        o_block(pair_far, h, 2, pair).wait_recv()
        at = pl.ds(h * o_rows, o_rows)
        total = hid[at, :].astype(jnp.float32)
        for part_o, part_w in ((o_in.at[at], wo_own), (o_full.at[far, at], wo_peer),
                               (o_full.at[pair, at], wo_pair), (o_full.at[pair_far, at], wo_pair_far)):
            total = total + jnp.dot(part_o[...], part_w[...], preferred_element_type=jnp.float32)
        x1[at, :] = total.astype(jnp.bfloat16)

    def routed(at, size):
        h2[at:at + size, :] = normed(x1[at:at + size, :].astype(jnp.float32), gain[...].astype(jnp.float32))
        logits = lax.dot_general(router[...], h2[at:at + size, :], (((1,), (1,)), ((), ())), preferred_element_type=jnp.float32)
        expert_id = lax.broadcasted_iota(jnp.int32, logits.shape, 0)
        picks = chosen[:, at:at + size]
        hit = expert_id == picks[0:1]
        for k in range(1, picks.shape[0]):
            hit = jnp.logical_or(hit, expert_id == picks[k:k + 1])
        shown = jnp.where(hit, logits, MASK_FILL)
        e = jnp.where(hit, jnp.exp(shown - jnp.max(shown, axis=0, keepdims=True)), 0.0)
        g = e / jnp.sum(e, axis=0, keepdims=True)
        gates[at:at + size, :] = jnp.concatenate([g, jnp.zeros((128 - experts, size), jnp.float32)], axis=0).T

    lane = lax.broadcasted_iota(jnp.int32, (block, 128), 1)

    def inner(p, lo, hi):
        def several(i, carry):
            for k in range(UNROLL):
                if p == 0 and k % GROUP == 0:
                    for copy in load_in(i * (UNROLL // GROUP) + k // GROUP):
                        copy.wait()
                e = i * UNROLL + k
                both = jnp.dot(h2[p * block:(p + 1) * block, :], w_in[e], preferred_element_type=jnp.float32)
                gate, up = both[:, :part], both[:, part:]
                weight = jnp.sum(jnp.where(lane == e, gates[p * block:(p + 1) * block, :], 0.0), axis=1, keepdims=True)
                act = weight * (gate / (1.0 + jnp.exp(-gate))) * up
                z[:, pl.ds(pl.multiple_of(e * part, part), part)] = act.astype(jnp.bfloat16)
            return carry
        lax.fori_loop(lo // UNROLL, hi // UNROLL, several, 0)

    def down(p, c):
        acc[p, c] = jnp.dot(z[...], w_dn[:, c * cols:(c + 1) * cols], preferred_element_type=jnp.float32)
        go(pair_copy(p, c))

    def direct(p, c):
        return p * CHUNKS + c >= PARTS * CHUNKS - DIRECT

    def pair_copy(p, c):
        return remote(acc.at[p, c, pl.ds((1 - core) * (block // 2), block // 2)], from_pair.at[p, c], a_snd.at[p, c], a_rcv.at[p, c], pair)

    def far_copy(p, c):
        if direct(p, c):
            return remote(chip_sum.at[p, c], from_far.at[p, c], b_snd.at[p, c], b_rcv.at[p, c], far)
        size = block // 4
        return remote(chip_sum.at[p, c, pl.ds((1 - chip) * size, size)], from_far.at[p, c, 0:size], b_snd.at[p, c], b_rcv.at[p, c], far)

    def out_copy(p, c, kind, of_core, of_chip, to):
        if direct(p, c):
            at = pl.ds(p * block + of_core * (block // 2), block // 2)
        else:
            at = pl.ds(p * block + of_core * (block // 2) + of_chip * (block // 4), block // 4)
        ref = out.at[at, c * cols:(c + 1) * cols]
        return remote(ref, ref, c_snd.at[kind, p, c], c_rcv.at[kind, p, c], to)

    def stage_b(p, c):
        pair_copy(p, c).wait_recv()
        chip_sum[p, c] = acc[p, c, pl.ds(core * (block // 2), block // 2)] + from_pair[p, c]
        go(far_copy(p, c))

    def stage_c(p, c):
        far_copy(p, c).wait_recv()
        cut = slice(c * cols, (c + 1) * cols)
        base = p * block + core * (block // 2)
        if direct(p, c):
            at = pl.ds(base, block // 2)
            total = chip_sum[p, c] + from_far[p, c]
        else:
            at = pl.ds(base + chip * (block // 4), block // 4)
            total = chip_sum[p, c, pl.ds(chip * (block // 4), block // 4)] + from_far[p, c, 0:block // 4]
        out[at, cut] = (x1[at, cut].astype(jnp.float32) + total).astype(jnp.bfloat16)
        if not direct(p, c):
            go(out_copy(p, c, 0, core, chip, far))
        go(out_copy(p, c, 1, core, chip, pair))

    def stage_d(p, c):
        if not direct(p, c):
            out_copy(p, c, 0, core, 1 - chip, far).wait_recv()
            go(out_copy(p, c, 2, core, 1 - chip, pair))

    def stage_e(p, c):
        out_copy(p, c, 1, 1 - core, chip, pair).wait_recv()
        if not direct(p, c):
            out_copy(p, c, 2, 1 - core, 1 - chip, pair).wait_recv()

    relay_o(0)
    for copy in wo_copies:
        copy.wait_recv()
    mid(0)
    if PARTS == 2:
        routed(0, block)
    relay_o(1)
    units = [(p, c) for p in range(PARTS) for c in range(CHUNKS)]
    if PARTS == 1:
        mid(1)
        routed(0, o_rows)
        routed(o_rows, o_rows)
        inner(0, 0, experts)
        for g in range(4):
            load_down(g).wait()
        for c in range(CHUNKS):
            down(0, c)
            if c >= 2:
                stage_b(0, c - 2)
        for c in range(max(CHUNKS - 2, 0), CHUNKS):
            stage_b(0, c)
        rest = units
    else:
        inner(0, 0, experts)
        for g in range(4):
            load_down(g).wait()
        for c in range(CHUNKS):
            down(0, c)
        mid(1)
        routed(block, block)
        for c in range(CHUNKS):
            stage_b(0, c)
        inner(1, 0, experts)
        for c in range(CHUNKS):
            down(1, c)
        for c in range(CHUNKS):
            stage_c(0, c)
        for c in range(CHUNKS):
            stage_b(1, c)
        rest = [(1, c) for c in range(CHUNKS)]
        for c in range(CHUNKS):
            stage_d(0, c)
    for unit in rest:
        stage_c(*unit)
    for unit in rest:
        stage_d(*unit)
    for unit in units:
        stage_e(*unit)
    for copy in sends:
        copy.wait_send()


def expert_call(o, hidden_in, chosen_t, g_moe, router_t, w_o, wo_peer, w_gate, w_up, w_down):
    rows, dim = hidden_in.shape
    experts, _, part = w_gate.shape
    block, cols = rows // PARTS, dim // CHUNKS
    any_spec = pl.BlockSpec(memory_space=pltpu.HBM)
    vmem = pl.BlockSpec(memory_space=pltpu.VMEM)
    dma = pltpu.SemaphoreType.DMA
    bf, f32 = jnp.bfloat16, jnp.float32
    return pl.pallas_call(
        expert_kernel,
        out_shape=jax.ShapeDtypeStruct((rows, dim), bf),
        in_specs=[vmem] * 7 + [any_spec] * 3,
        out_specs=vmem,
        scratch_shapes=[
            pltpu.VMEM(w_o.shape, bf),
            pltpu.VMEM(w_o.shape, bf),
            pltpu.VMEM((4,) + o.shape, bf),
            pltpu.VMEM((experts, dim, 2 * part), bf),
            pltpu.VMEM((experts * part, dim), bf),
            pltpu.VMEM((rows, dim), bf),
            pltpu.VMEM((rows, dim), bf),
            pltpu.VMEM((rows, 128), f32),
            pltpu.VMEM((block, experts * part), bf),
            pltpu.VMEM((PARTS, CHUNKS, block, cols), f32),
            pltpu.VMEM((PARTS, CHUNKS, block // 2, cols), f32),
            pltpu.VMEM((PARTS, CHUNKS, block // 2, cols), f32),
            pltpu.VMEM((PARTS, CHUNKS, block // 2, cols), f32),
            dma((2, experts // GROUP)), dma((4,)), dma((2,)), dma((2,)), dma((3, 2)), dma((3, 2)),
            dma((PARTS, CHUNKS)), dma((PARTS, CHUNKS)), dma((PARTS, CHUNKS)), dma((PARTS, CHUNKS)),
            dma((3, PARTS, CHUNKS)), dma((3, PARTS, CHUNKS)),
        ],
        compiler_params=pltpu.CompilerParams(collective_id=0, has_side_effects=True, vmem_limit_bytes=40 << 20),
        cost_estimate=pl.CostEstimate(flops=7 * 10**9, bytes_accessed=28 * 10**6, transcendentals=0),
        name="experts",
    )(o, chosen_t, g_moe, router_t, hidden_in, w_o, wo_peer, *(pinned(w) for w in (w_gate, w_up, w_down.reshape(experts * part, dim))))


def solution(mesh):
    cache_spec = P("dp", None, "tp", None)
    in_specs = (P("dp", None), cache_spec, cache_spec, P("dp"), P("dp", None), P(None), P(None, "tp"), P(None, "tp"), P(None, "tp"), P("tp", None), P(None), P(None, None), P(None, None, "tp"), P(None, None, "tp"), P(None, "tp", None))
    out_specs = (P("dp", None), cache_spec, cache_spec)

    def layer_shard(hidden_in, k_cache, v_cache, seq_lens, chosen_experts, g_attn, w_q, w_k, w_v, w_o, g_moe, w_router, w_gate, w_up, w_down):
        rows, slots, kvh, hd = k_cache.shape
        as_t = lambda c: c.transpose(0, 2, 3, 1).reshape(rows, kvh * hd, slots)
        back = lambda c: c.reshape(rows, kvh, hd, slots).transpose(0, 3, 1, 2)
        wo_peer = lax.ppermute(w_o, "tp", [(0, 2), (1, 3), (2, 0), (3, 1)])
        o, k_n, v_n = attention_call(hidden_in, as_t(k_cache), as_t(v_cache), seq_lens, g_attn, w_q, w_k, w_v)
        hidden_out = expert_call(o, hidden_in, chosen_experts.T, g_moe, w_router.T, w_o, wo_peer, w_gate, w_up, w_down)
        return hidden_out, back(k_n), back(v_n)

    return jax.shard_map(layer_shard, mesh=mesh, in_specs=in_specs, out_specs=out_specs, check_vma=False)
```

```python
import math
import jax
import jax.numpy as jnp
from jax import lax
from jax.experimental import pallas as pl
from jax.experimental.pallas import tpu as pltpu
from jax.sharding import PartitionSpec as P

EPSILON = 1e-5
ROPE_THETA = 1000000.0
MASK_FILL = -1e30
BLOCK = 16
SLOTS = 8
AHEAD = 2
FIRST = 2
GROUP = 4
UNROLL = 16
PARTS = 2
CHUNKS = 2
DIRECT = 1


def pinned(array):
    return pltpu.with_memory_space_constraint(array, pltpu.HBM)


def normed(vector32, gain32):
    scale = lax.rsqrt(jnp.mean(vector32 * vector32, axis=-1, keepdims=True) + EPSILON)
    return (vector32 * scale * gain32).astype(jnp.bfloat16)


def attention_kernel(seq_lens, g_attn, hidden, w_q, w_k, w_v, k_in, v_in, o_out, k_out, v_out,
                     seq_s, seq_v, gain, hid, wqkv, kv_col, q_rows, o_rows, kbuf, vbuf, w_sem, k_rd, v_rd, k_wr, v_wr):
    rows, width, slots = k_in.shape
    heads_w = w_q.shape[1]
    half = width // 4
    steps = rows // BLOCK

    def read(i, slot):
        src = pl.ds(i * BLOCK, BLOCK)
        return (pltpu.make_async_copy(k_in.at[src], kbuf.at[slot], k_rd.at[slot]),
                pltpu.make_async_copy(v_in.at[src], vbuf.at[slot], v_rd.at[slot]))

    def write(i, slot):
        dst = pl.ds(i * BLOCK, BLOCK)
        return (pltpu.make_async_copy(kbuf.at[slot], k_out.at[dst], k_wr.at[slot]),
                pltpu.make_async_copy(vbuf.at[slot], v_out.at[dst], v_wr.at[slot]))

    loads = [pltpu.make_async_copy(hidden, hid, w_sem.at[0]),
             pltpu.make_async_copy(w_q, wqkv.at[:, 0:heads_w], w_sem.at[1]),
             pltpu.make_async_copy(w_k, wqkv.at[:, heads_w:heads_w + width], w_sem.at[2]),
             pltpu.make_async_copy(w_v, wqkv.at[:, heads_w + width:], w_sem.at[3]),
             pltpu.make_async_copy(seq_lens, seq_v, w_sem.at[4]),
             pltpu.make_async_copy(seq_lens, seq_s, w_sem.at[5]),
             pltpu.make_async_copy(g_attn, gain, w_sem.at[6])]
    for copy in loads:
        copy.start()
    for i in range(FIRST):
        for copy in read(i, i):
            copy.start()
    loads[4].wait()
    place = lax.broadcasted_iota(jnp.int32, (half, rows), 0).astype(jnp.float32)
    angles = jnp.exp(place * (-math.log(ROPE_THETA) / half)) * seq_v[...].astype(jnp.float32)[None, :]
    cos_t, sin_t = jnp.cos(angles), jnp.sin(angles)
    for copy in loads[:4] + loads[5:]:
        copy.wait()
    for i in range(FIRST, SLOTS):
        for copy in read(i, i):
            copy.start()
    h = normed(hid[...].astype(jnp.float32), gain[...].astype(jnp.float32))
    qkv_t = jnp.dot(h, wqkv[...], preferred_element_type=jnp.float32).T

    def rotated(at):
        a, c = qkv_t[at:at + half], qkv_t[at + half:at + 2 * half]
        return [a * cos_t - c * sin_t, c * cos_t + a * sin_t]

    k_t = jnp.concatenate(rotated(heads_w) + rotated(heads_w + 2 * half), axis=0)
    v_t = qkv_t[heads_w + width:]
    for part in range(rows // 128):
        lanes = slice(part * 128, part * 128 + 128)
        kv_col[part, 0:width] = k_t[:, lanes].astype(jnp.bfloat16)
        kv_col[part, width:] = v_t[:, lanes].astype(jnp.bfloat16)
    lane = lax.broadcasted_iota(jnp.int32, (rows, width), 1)
    for g in range(2):
        q_g = jnp.concatenate(rotated(g * 2 * half) + rotated((2 + g) * 2 * half), axis=0).T
        q_g = q_g.astype(jnp.bfloat16).astype(jnp.float32) * 0.125
        for kv in range(2):
            keep = (lane < 2 * half) if kv == 0 else (lane >= 2 * half)
            q_rows[pl.ds(kv * 2 + g, rows, stride=8), :] = jnp.where(keep, q_g, 0.0)
    for r in range(4, 8):
        q_rows[pl.ds(r, rows, stride=8), :] = jnp.zeros((rows, width), jnp.float32)

    slot_id = lax.broadcasted_iota(jnp.int32, (8, slots), 1)
    slot_bf = lax.broadcasted_iota(jnp.int32, (width, 128), 1).astype(jnp.float32).astype(jnp.bfloat16)

    row_id = lax.broadcasted_iota(jnp.int32, (128, 256), 0) - lax.div(lax.broadcasted_iota(jnp.int32, (128, 256), 1), 128)
    row_bf = row_id.astype(jnp.float32).astype(jnp.bfloat16)

    def step(i, carry):
        slot = lax.rem(i, SLOTS)
        for copy in read(i, slot):
            copy.wait()
        per = 128 // BLOCK
        columns = kv_col[lax.div(i, per)]
        first_row = lax.rem(i, per) * BLOCK
        cols = []
        for j in range(0, BLOCK, 2):
            pick = (row_bf == (first_row + j).astype(jnp.float32).astype(jnp.bfloat16))
            pick = jnp.where(pick, jnp.ones((), jnp.bfloat16), jnp.zeros((), jnp.bfloat16))
            both = jnp.dot(columns, pick, preferred_element_type=jnp.float32).astype(jnp.bfloat16)
            cols += [both[:, 0:128], both[:, 128:256]]
        places = [seq_s[i * BLOCK + j] for j in range(BLOCK)]

        def updated(buf, j, at):
            side = pl.ds(pl.multiple_of(lax.div(places[j], 128) * 128, 128), 128)
            here = slot_bf == lax.rem(places[j], 128).astype(jnp.float32).astype(jnp.bfloat16)
            buf[slot, j, :, side] = jnp.where(here, cols[j][at:at + width], buf[slot, j, :, side])
            return buf[slot, j]

        scores = []
        for j in range(BLOCK):
            q = q_rows[pl.ds((i * BLOCK + j) * 8, 8), :].astype(jnp.bfloat16)
            s = jnp.dot(q, updated(kbuf, j, 0), preferred_element_type=jnp.float32)
            scores.append(jnp.where(slot_id <= places[j], s, MASK_FILL))
        for j in range(BLOCK):
            s = scores[j]
            e = jnp.exp(s - jnp.max(s, axis=-1, keepdims=True))
            w = (e / jnp.sum(e, axis=-1, keepdims=True)).astype(jnp.bfloat16)
            o = lax.dot_general(w, updated(vbuf, j, width), (((1,), (1,)), ((), ())), preferred_element_type=jnp.float32)
            o_rows[pl.ds(j * 8, 8), :] = o
        for copy in write(i, slot):
            copy.start()
        low = lax.broadcasted_iota(jnp.int32, (BLOCK, width), 1) < 2 * half
        for kv in range(2):
            first = o_rows[pl.ds(2 * kv, BLOCK, stride=8), :]
            second = o_rows[pl.ds(2 * kv + 1, BLOCK, stride=8), :]
            if kv == 0:
                second = pltpu.roll(second, 2 * half, axis=1)
            else:
                first = pltpu.roll(first, 2 * half, axis=1)
            o_out[pl.ds(i * BLOCK, BLOCK), kv * width:(kv + 1) * width] = jnp.where(low, first, second).astype(jnp.bfloat16)

        @pl.when(jnp.logical_and(i >= AHEAD, i < steps - SLOTS + AHEAD))
        def _():
            old = lax.rem(i + SLOTS - AHEAD, SLOTS)
            for copy in write(i - AHEAD, old):
                copy.wait()
            for copy in read(i + SLOTS - AHEAD, old):
                copy.start()
        return carry

    lax.fori_loop(0, steps, step, 0)
    for i in range(steps - SLOTS, steps):
        for copy in write(i, i % SLOTS):
            copy.wait()


def attention_call(hidden_in, k_t, v_t, seq_lens, g_attn, w_q, w_k, w_v):
    rows, width, slots = k_t.shape
    any_spec = pl.BlockSpec(memory_space=pltpu.HBM)
    vmem = pl.BlockSpec(memory_space=pltpu.VMEM)
    cache = jax.ShapeDtypeStruct(k_t.shape, k_t.dtype)
    dma = pltpu.SemaphoreType.DMA
    return pl.pallas_call(
        attention_kernel,
        out_shape=(jax.ShapeDtypeStruct((rows, w_q.shape[1]), jnp.bfloat16), cache, cache),
        in_specs=[any_spec] * 8,
        out_specs=(vmem, any_spec, any_spec),
        scratch_shapes=[
            pltpu.SMEM(seq_lens.shape, jnp.int32),
            pltpu.VMEM(seq_lens.shape, jnp.int32),
            pltpu.VMEM(g_attn.shape, jnp.bfloat16),
            pltpu.VMEM(hidden_in.shape, jnp.bfloat16),
            pltpu.VMEM((hidden_in.shape[1], w_q.shape[1] + 2 * width), jnp.bfloat16),
            pltpu.VMEM((rows // 128, 2 * width, 128), jnp.bfloat16),
            pltpu.VMEM((rows * 8, width), jnp.float32),
            pltpu.VMEM((BLOCK * 8, width), jnp.float32),
            pltpu.VMEM((SLOTS, BLOCK, width, slots), jnp.bfloat16),
            pltpu.VMEM((SLOTS, BLOCK, width, slots), jnp.bfloat16),
            dma((7,)), dma((SLOTS,)), dma((SLOTS,)), dma((SLOTS,)), dma((SLOTS,)),
        ],
        compiler_params=pltpu.CompilerParams(vmem_limit_bytes=26 << 20),
        cost_estimate=pl.CostEstimate(flops=10**9, bytes_accessed=70 * 10**6, transcendentals=0),
        name="attention",
    )(*(pinned(a) for a in (seq_lens, g_attn, hidden_in, w_q, w_k, w_v, k_t, v_t)))


def expert_kernel(o_in, chosen, gain, router, hid, wo_own, wo_peer, w_gate, w_up, w_down, out,
                  wo_pair, wo_pair_far, o_full, w_in, w_dn, x1, h2, gates, z, acc, from_pair, chip_sum, from_far,
                  wi_sem, wd_sem, wo_snd, wo_rcv, o_snd, o_rcv, a_snd, a_rcv, b_snd, b_rcv, c_snd, c_rcv):
    experts, dim, part = w_gate.shape
    rows = hid.shape[0]
    o_rows = rows // 2
    block = rows // PARTS
    cols = dim // CHUNKS
    groups = experts // GROUP
    me = lax.axis_index("tp")
    core, chip = lax.rem(me, 2), lax.div(me, 2)
    pair, far = me + 1 - 2 * core, me + 2 - 4 * chip
    pair_far = far + 1 - 2 * core

    def remote(src, dst, send, recv, to):
        return pltpu.make_async_remote_copy(src_ref=src, dst_ref=dst, send_sem=send, recv_sem=recv,
                                            device_id={"tp": to}, device_id_type=pl.DeviceIdType.MESH)

    def load_in(g):
        sl = pl.ds(g * GROUP, GROUP)
        return (pltpu.make_async_copy(w_gate.at[sl], w_in.at[sl, :, 0:part], wi_sem.at[0, g]),
                pltpu.make_async_copy(w_up.at[sl], w_in.at[sl, :, part:2 * part], wi_sem.at[1, g]))

    def load_down(g):
        sl = pl.ds(g * (w_dn.shape[0] // 4), w_dn.shape[0] // 4)
        return pltpu.make_async_copy(w_down.at[sl], w_dn.at[sl], wd_sem.at[g])

    barrier = pltpu.get_barrier_semaphore()
    for peer in (pair, far):
        pl.semaphore_signal(barrier, inc=1, device_id={"tp": peer}, device_id_type=pl.DeviceIdType.MESH)
    for g in range(groups):
        for copy in load_in(g):
            copy.start()
    pl.semaphore_wait(barrier, 2)

    def o_block(owner, h, kind, to):
        at = pl.ds(h * o_rows, o_rows)
        src = o_in.at[at] if kind < 2 else o_full.at[owner, at]
        return remote(src, o_full.at[owner, at], o_snd.at[kind, h], o_rcv.at[kind, h], to)

    sends = []

    def go(copy):
        copy.start()
        sends.append(copy)

    wo_copies = [remote(wo_own, wo_pair, wo_snd.at[0], wo_rcv.at[0], pair),
                 remote(wo_peer, wo_pair_far, wo_snd.at[1], wo_rcv.at[1], pair)]
    for h in range(2):
        go(o_block(me, h, 0, far))
    for h in range(2):
        go(o_block(me, h, 1, pair))
    for copy in wo_copies:
        go(copy)

    def relay_o(h):
        o_block(far, h, 0, far).wait_recv()
        go(o_block(far, h, 2, pair))

    def mid(h):
        o_block(pair, h, 1, pair).wait_recv()
        o_block(pair_far, h, 2, pair).wait_recv()
        at = pl.ds(h * o_rows, o_rows)
        total = hid[at, :].astype(jnp.float32)
        for part_o, part_w in ((o_in.at[at], wo_own), (o_full.at[far, at], wo_peer),
                               (o_full.at[pair, at], wo_pair), (o_full.at[pair_far, at], wo_pair_far)):
            total = total + jnp.dot(part_o[...], part_w[...], preferred_element_type=jnp.float32)
        x1[at, :] = total.astype(jnp.bfloat16)

    def routed(at, size):
        h2[at:at + size, :] = normed(x1[at:at + size, :].astype(jnp.float32), gain[...].astype(jnp.float32))
        logits = lax.dot_general(router[...], h2[at:at + size, :], (((1,), (1,)), ((), ())), preferred_element_type=jnp.float32)
        expert_id = lax.broadcasted_iota(jnp.int32, logits.shape, 0)
        picks = chosen[:, at:at + size]
        hit = expert_id == picks[0:1]
        for k in range(1, picks.shape[0]):
            hit = jnp.logical_or(hit, expert_id == picks[k:k + 1])
        shown = jnp.where(hit, logits, MASK_FILL)
        e = jnp.where(hit, jnp.exp(shown - jnp.max(shown, axis=0, keepdims=True)), 0.0)
        g = e / jnp.sum(e, axis=0, keepdims=True)
        gates[at:at + size, :] = jnp.concatenate([g, jnp.zeros((128 - experts, size), jnp.float32)], axis=0).T

    lane = lax.broadcasted_iota(jnp.int32, (block, 128), 1)

    def inner(p, lo, hi):
        def several(i, carry):
            for k in range(UNROLL):
                if p == 0 and k % GROUP == 0:
                    for copy in load_in(i * (UNROLL // GROUP) + k // GROUP):
                        copy.wait()
                e = i * UNROLL + k
                both = jnp.dot(h2[p * block:(p + 1) * block, :], w_in[e], preferred_element_type=jnp.float32)
                gate, up = both[:, :part], both[:, part:]
                weight = jnp.sum(jnp.where(lane == e, gates[p * block:(p + 1) * block, :], 0.0), axis=1, keepdims=True)
                act = weight * (gate / (1.0 + jnp.exp(-gate))) * up
                z[:, pl.ds(pl.multiple_of(e * part, part), part)] = act.astype(jnp.bfloat16)
            return carry
        lax.fori_loop(lo // UNROLL, hi // UNROLL, several, 0)

    def down(p, c):
        acc[p, c] = jnp.dot(z[...], w_dn[:, c * cols:(c + 1) * cols], preferred_element_type=jnp.float32)
        go(pair_copy(p, c))

    def direct(p, c):
        return p * CHUNKS + c >= PARTS * CHUNKS - DIRECT

    def pair_copy(p, c):
        return remote(acc.at[p, c, pl.ds((1 - core) * (block // 2), block // 2)], from_pair.at[p, c], a_snd.at[p, c], a_rcv.at[p, c], pair)

    def far_copy(p, c):
        if direct(p, c):
            return remote(chip_sum.at[p, c], from_far.at[p, c], b_snd.at[p, c], b_rcv.at[p, c], far)
        size = block // 4
        return remote(chip_sum.at[p, c, pl.ds((1 - chip) * size, size)], from_far.at[p, c, 0:size], b_snd.at[p, c], b_rcv.at[p, c], far)

    def out_copy(p, c, kind, of_core, of_chip, to):
        if direct(p, c):
            at = pl.ds(p * block + of_core * (block // 2), block // 2)
        else:
            at = pl.ds(p * block + of_core * (block // 2) + of_chip * (block // 4), block // 4)
        ref = out.at[at, c * cols:(c + 1) * cols]
        return remote(ref, ref, c_snd.at[kind, p, c], c_rcv.at[kind, p, c], to)

    def stage_b(p, c):
        pair_copy(p, c).wait_recv()
        chip_sum[p, c] = acc[p, c, pl.ds(core * (block // 2), block // 2)] + from_pair[p, c]
        go(far_copy(p, c))

    def stage_c(p, c):
        far_copy(p, c).wait_recv()
        cut = slice(c * cols, (c + 1) * cols)
        base = p * block + core * (block // 2)
        if direct(p, c):
            at = pl.ds(base, block // 2)
            total = chip_sum[p, c] + from_far[p, c]
        else:
            at = pl.ds(base + chip * (block // 4), block // 4)
            total = chip_sum[p, c, pl.ds(chip * (block // 4), block // 4)] + from_far[p, c, 0:block // 4]
        out[at, cut] = (x1[at, cut].astype(jnp.float32) + total).astype(jnp.bfloat16)
        if not direct(p, c):
            go(out_copy(p, c, 0, core, chip, far))
        go(out_copy(p, c, 1, core, chip, pair))

    def stage_d(p, c):
        if not direct(p, c):
            out_copy(p, c, 0, core, 1 - chip, far).wait_recv()
            go(out_copy(p, c, 2, core, 1 - chip, pair))

    def stage_e(p, c):
        out_copy(p, c, 1, 1 - core, chip, pair).wait_recv()
        if not direct(p, c):
            out_copy(p, c, 2, 1 - core, 1 - chip, pair).wait_recv()

    relay_o(0)
    for g in range(4):
        load_down(g).start()
    for copy in wo_copies:
        copy.wait_recv()
    mid(0)
    if PARTS == 2:
        routed(0, block)
    relay_o(1)
    units = [(p, c) for p in range(PARTS) for c in range(CHUNKS)]
    if PARTS == 1:
        mid(1)
        routed(0, o_rows)
        routed(o_rows, o_rows)
        inner(0, 0, experts)
        for g in range(4):
            load_down(g).wait()
        for c in range(CHUNKS):
            down(0, c)
            if c >= 2:
                stage_b(0, c - 2)
        for c in range(max(CHUNKS - 2, 0), CHUNKS):
            stage_b(0, c)
        rest = units
    else:
        inner(0, 0, experts)
        for g in range(4):
            load_down(g).wait()
        for c in range(CHUNKS):
            down(0, c)
        mid(1)
        routed(block, block)
        for c in range(CHUNKS):
            stage_b(0, c)
        inner(1, 0, experts)
        for c in range(CHUNKS):
            down(1, c)
            if c < CHUNKS - 1:
                stage_c(0, c)
        stage_b(1, 0)
        stage_c(0, CHUNKS - 1)
        for c in range(1, CHUNKS):
            stage_b(1, c)
        rest = [(1, c) for c in range(CHUNKS)]
        for c in range(CHUNKS):
            stage_d(0, c)
    for unit in rest:
        stage_c(*unit)
    for unit in rest:
        stage_d(*unit)
    for unit in units:
        stage_e(*unit)
    for copy in sends:
        copy.wait_send()


def expert_call(o, hidden_in, chosen_t, g_moe, router_t, w_o, wo_peer, w_gate, w_up, w_down):
    rows, dim = hidden_in.shape
    experts, _, part = w_gate.shape
    block, cols = rows // PARTS, dim // CHUNKS
    any_spec = pl.BlockSpec(memory_space=pltpu.HBM)
    vmem = pl.BlockSpec(memory_space=pltpu.VMEM)
    dma = pltpu.SemaphoreType.DMA
    bf, f32 = jnp.bfloat16, jnp.float32
    return pl.pallas_call(
        expert_kernel,
        out_shape=jax.ShapeDtypeStruct((rows, dim), bf),
        in_specs=[vmem] * 7 + [any_spec] * 3,
        out_specs=vmem,
        scratch_shapes=[
            pltpu.VMEM(w_o.shape, bf),
            pltpu.VMEM(w_o.shape, bf),
            pltpu.VMEM((4,) + o.shape, bf),
            pltpu.VMEM((experts, dim, 2 * part), bf),
            pltpu.VMEM((experts * part, dim), bf),
            pltpu.VMEM((rows, dim), bf),
            pltpu.VMEM((rows, dim), bf),
            pltpu.VMEM((rows, 128), f32),
            pltpu.VMEM((block, experts * part), bf),
            pltpu.VMEM((PARTS, CHUNKS, block, cols), f32),
            pltpu.VMEM((PARTS, CHUNKS, block // 2, cols), f32),
            pltpu.VMEM((PARTS, CHUNKS, block // 2, cols), f32),
            pltpu.VMEM((PARTS, CHUNKS, block // 2, cols), f32),
            dma((2, experts // GROUP)), dma((4,)), dma((2,)), dma((2,)), dma((3, 2)), dma((3, 2)),
            dma((PARTS, CHUNKS)), dma((PARTS, CHUNKS)), dma((PARTS, CHUNKS)), dma((PARTS, CHUNKS)),
            dma((3, PARTS, CHUNKS)), dma((3, PARTS, CHUNKS)),
        ],
        compiler_params=pltpu.CompilerParams(collective_id=0, has_side_effects=True, vmem_limit_bytes=40 << 20),
        cost_estimate=pl.CostEstimate(flops=7 * 10**9, bytes_accessed=28 * 10**6, transcendentals=0),
        name="experts",
    )(o, chosen_t, g_moe, router_t, hidden_in, w_o, wo_peer, *(pinned(w) for w in (w_gate, w_up, w_down.reshape(experts * part, dim))))


def solution(mesh):
    cache_spec = P("dp", None, "tp", None)
    in_specs = (P("dp", None), cache_spec, cache_spec, P("dp"), P("dp", None), P(None), P(None, "tp"), P(None, "tp"), P(None, "tp"), P("tp", None), P(None), P(None, None), P(None, None, "tp"), P(None, None, "tp"), P(None, "tp", None))
    out_specs = (P("dp", None), cache_spec, cache_spec)

    def layer_shard(hidden_in, k_cache, v_cache, seq_lens, chosen_experts, g_attn, w_q, w_k, w_v, w_o, g_moe, w_router, w_gate, w_up, w_down):
        rows, slots, kvh, hd = k_cache.shape
        as_t = lambda c: c.transpose(0, 2, 3, 1).reshape(rows, kvh * hd, slots)
        back = lambda c: c.reshape(rows, kvh, hd, slots).transpose(0, 3, 1, 2)
        wo_peer = lax.ppermute(w_o, "tp", [(0, 2), (1, 3), (2, 0), (3, 1)])
        o, k_n, v_n = attention_call(hidden_in, as_t(k_cache), as_t(v_cache), seq_lens, g_attn, w_q, w_k, w_v)
        hidden_out = expert_call(o, hidden_in, chosen_experts.T, g_moe, w_router.T, w_o, wo_peer, w_gate, w_up, w_down)
        return hidden_out, back(k_n), back(v_n)

    return jax.shard_map(layer_shard, mesh=mesh, in_specs=in_specs, out_specs=out_specs, check_vma=False)
```

```python
import math
import jax
import jax.numpy as jnp
from jax import lax
from jax.experimental import pallas as pl
from jax.experimental.pallas import tpu as pltpu
from jax.sharding import PartitionSpec as P

EPSILON = 1e-5
ROPE_THETA = 1000000.0
MASK_FILL = -1e30
BLOCK = 16
SLOTS = 8
AHEAD = 2
FIRST = 2
GROUP = 4
UNROLL = 16
PARTS = 2
CHUNKS = 2
DIRECT = 1


def pinned(array):
    return pltpu.with_memory_space_constraint(array, pltpu.HBM)


def normed(vector32, gain32):
    scale = lax.rsqrt(jnp.mean(vector32 * vector32, axis=-1, keepdims=True) + EPSILON)
    return (vector32 * scale * gain32).astype(jnp.bfloat16)


def attention_kernel(seq_lens, g_attn, hidden, w_q, w_k, w_v, k_in, v_in, o_out, k_out, v_out,
                     seq_s, seq_v, gain, hid, wqkv, kv_col, q_rows, o_rows, kbuf, vbuf, w_sem, k_rd, v_rd, k_wr, v_wr):
    rows, width, slots = k_in.shape
    heads_w = w_q.shape[1]
    half = width // 4
    steps = rows // BLOCK

    def read(i, slot):
        src = pl.ds(i * BLOCK, BLOCK)
        return (pltpu.make_async_copy(k_in.at[src], kbuf.at[slot], k_rd.at[slot]),
                pltpu.make_async_copy(v_in.at[src], vbuf.at[slot], v_rd.at[slot]))

    def write(i, slot):
        dst = pl.ds(i * BLOCK, BLOCK)
        return (pltpu.make_async_copy(kbuf.at[slot], k_out.at[dst], k_wr.at[slot]),
                pltpu.make_async_copy(vbuf.at[slot], v_out.at[dst], v_wr.at[slot]))

    loads = [pltpu.make_async_copy(hidden, hid, w_sem.at[0]),
             pltpu.make_async_copy(w_q, wqkv.at[:, 0:heads_w], w_sem.at[1]),
             pltpu.make_async_copy(w_k, wqkv.at[:, heads_w:heads_w + width], w_sem.at[2]),
             pltpu.make_async_copy(w_v, wqkv.at[:, heads_w + width:], w_sem.at[3]),
             pltpu.make_async_copy(seq_lens, seq_v, w_sem.at[4]),
             pltpu.make_async_copy(seq_lens, seq_s, w_sem.at[5]),
             pltpu.make_async_copy(g_attn, gain, w_sem.at[6])]
    for copy in loads:
        copy.start()
    for i in range(FIRST):
        for copy in read(i, i):
            copy.start()
    loads[4].wait()
    place = lax.broadcasted_iota(jnp.int32, (half, rows), 0).astype(jnp.float32)
    angles = jnp.exp(place * (-math.log(ROPE_THETA) / half)) * seq_v[...].astype(jnp.float32)[None, :]
    cos_t, sin_t = jnp.cos(angles), jnp.sin(angles)
    for copy in loads[:4] + loads[5:]:
        copy.wait()
    for i in range(FIRST, SLOTS):
        for copy in read(i, i):
            copy.start()
    h = normed(hid[...].astype(jnp.float32), gain[...].astype(jnp.float32))
    qkv_t = jnp.dot(h, wqkv[...], preferred_element_type=jnp.float32).T

    def rotated(at):
        a, c = qkv_t[at:at + half], qkv_t[at + half:at + 2 * half]
        return [a * cos_t - c * sin_t, c * cos_t + a * sin_t]

    k_t = jnp.concatenate(rotated(heads_w) + rotated(heads_w + 2 * half), axis=0)
    v_t = qkv_t[heads_w + width:]
    for part in range(rows // 128):
        lanes = slice(part * 128, part * 128 + 128)
        kv_col[part, 0:width] = k_t[:, lanes].astype(jnp.bfloat16)
        kv_col[part, width:] = v_t[:, lanes].astype(jnp.bfloat16)
    lane = lax.broadcasted_iota(jnp.int32, (rows, width), 1)
    for g in range(2):
        q_g = jnp.concatenate(rotated(g * 2 * half) + rotated((2 + g) * 2 * half), axis=0).T
        q_g = q_g.astype(jnp.bfloat16).astype(jnp.float32) * 0.125
        for kv in range(2):
            keep = (lane < 2 * half) if kv == 0 else (lane >= 2 * half)
            q_rows[pl.ds(kv * 2 + g, rows, stride=8), :] = jnp.where(keep, q_g, 0.0)
    for r in range(4, 8):
        q_rows[pl.ds(r, rows, stride=8), :] = jnp.zeros((rows, width), jnp.float32)

    slot_id = lax.broadcasted_iota(jnp.int32, (8, slots), 1)
    slot_bf = lax.broadcasted_iota(jnp.int32, (width, 128), 1).astype(jnp.float32).astype(jnp.bfloat16)

    row_id = lax.broadcasted_iota(jnp.int32, (128, 256), 0) - lax.div(lax.broadcasted_iota(jnp.int32, (128, 256), 1), 128)
    row_bf = row_id.astype(jnp.float32).astype(jnp.bfloat16)

    def step(i, carry):
        slot = lax.rem(i, SLOTS)
        for copy in read(i, slot):
            copy.wait()
        per = 128 // BLOCK
        columns = kv_col[lax.div(i, per)]
        first_row = lax.rem(i, per) * BLOCK
        cols = []
        for j in range(0, BLOCK, 2):
            pick = (row_bf == (first_row + j).astype(jnp.float32).astype(jnp.bfloat16))
            pick = jnp.where(pick, jnp.ones((), jnp.bfloat16), jnp.zeros((), jnp.bfloat16))
            both = jnp.dot(columns, pick, preferred_element_type=jnp.float32).astype(jnp.bfloat16)
            cols += [both[:, 0:128], both[:, 128:256]]
        places = [seq_s[i * BLOCK + j] for j in range(BLOCK)]

        def updated(buf, j, at):
            side = pl.ds(pl.multiple_of(lax.div(places[j], 128) * 128, 128), 128)
            here = slot_bf == lax.rem(places[j], 128).astype(jnp.float32).astype(jnp.bfloat16)
            buf[slot, j, :, side] = jnp.where(here, cols[j][at:at + width], buf[slot, j, :, side])
            return buf[slot, j]

        scores = []
        for j in range(BLOCK):
            q = q_rows[pl.ds((i * BLOCK + j) * 8, 8), :].astype(jnp.bfloat16)
            s = jnp.dot(q, updated(kbuf, j, 0), preferred_element_type=jnp.float32)
            scores.append(jnp.where(slot_id <= places[j], s, MASK_FILL))
        for j in range(BLOCK):
            s = scores[j]
            e = jnp.exp(s - jnp.max(s, axis=-1, keepdims=True))
            w = (e / jnp.sum(e, axis=-1, keepdims=True)).astype(jnp.bfloat16)
            o = lax.dot_general(w, updated(vbuf, j, width), (((1,), (1,)), ((), ())), preferred_element_type=jnp.float32)
            o_rows[pl.ds(j * 8, 8), :] = o
        for copy in write(i, slot):
            copy.start()
        low = lax.broadcasted_iota(jnp.int32, (BLOCK, width), 1) < 2 * half
        for kv in range(2):
            first = o_rows[pl.ds(2 * kv, BLOCK, stride=8), :]
            second = o_rows[pl.ds(2 * kv + 1, BLOCK, stride=8), :]
            if kv == 0:
                second = pltpu.roll(second, 2 * half, axis=1)
            else:
                first = pltpu.roll(first, 2 * half, axis=1)
            o_out[pl.ds(i * BLOCK, BLOCK), kv * width:(kv + 1) * width] = jnp.where(low, first, second).astype(jnp.bfloat16)

        @pl.when(jnp.logical_and(i >= AHEAD, i < steps - SLOTS + AHEAD))
        def _():
            old = lax.rem(i + SLOTS - AHEAD, SLOTS)
            for copy in write(i - AHEAD, old):
                copy.wait()
            for copy in read(i + SLOTS - AHEAD, old):
                copy.start()
        return carry

    lax.fori_loop(0, steps, step, 0)
    for i in range(steps - SLOTS, steps):
        for copy in write(i, i % SLOTS):
            copy.wait()


def attention_call(hidden_in, k_t, v_t, seq_lens, g_attn, w_q, w_k, w_v):
    rows, width, slots = k_t.shape
    any_spec = pl.BlockSpec(memory_space=pltpu.HBM)
    vmem = pl.BlockSpec(memory_space=pltpu.VMEM)
    cache = jax.ShapeDtypeStruct(k_t.shape, k_t.dtype)
    dma = pltpu.SemaphoreType.DMA
    return pl.pallas_call(
        attention_kernel,
        out_shape=(jax.ShapeDtypeStruct((rows, w_q.shape[1]), jnp.bfloat16), cache, cache),
        in_specs=[any_spec] * 8,
        out_specs=(vmem, any_spec, any_spec),
        scratch_shapes=[
            pltpu.SMEM(seq_lens.shape, jnp.int32),
            pltpu.VMEM(seq_lens.shape, jnp.int32),
            pltpu.VMEM(g_attn.shape, jnp.bfloat16),
            pltpu.VMEM(hidden_in.shape, jnp.bfloat16),
            pltpu.VMEM((hidden_in.shape[1], w_q.shape[1] + 2 * width), jnp.bfloat16),
            pltpu.VMEM((rows // 128, 2 * width, 128), jnp.bfloat16),
            pltpu.VMEM((rows * 8, width), jnp.float32),
            pltpu.VMEM((BLOCK * 8, width), jnp.float32),
            pltpu.VMEM((SLOTS, BLOCK, width, slots), jnp.bfloat16),
            pltpu.VMEM((SLOTS, BLOCK, width, slots), jnp.bfloat16),
            dma((7,)), dma((SLOTS,)), dma((SLOTS,)), dma((SLOTS,)), dma((SLOTS,)),
        ],
        compiler_params=pltpu.CompilerParams(vmem_limit_bytes=26 << 20),
        cost_estimate=pl.CostEstimate(flops=10**9, bytes_accessed=70 * 10**6, transcendentals=0),
        name="attention",
    )(*(pinned(a) for a in (seq_lens, g_attn, hidden_in, w_q, w_k, w_v, k_t, v_t)))


def expert_kernel(o_in, chosen, gain, router, hid, wo_own, wo_peer, w_gate, w_up, w_down, out,
                  wo_pair, wo_pair_far, o_full, w_in, w_dn, x1, h2, gates, z, acc, from_pair, chip_sum, from_far,
                  wi_sem, wd_sem, wo_snd, wo_rcv, o_snd, o_rcv, a_snd, a_rcv, b_snd, b_rcv, c_snd, c_rcv):
    experts, dim, part = w_gate.shape
    rows = hid.shape[0]
    o_rows = rows // 2
    block = rows // PARTS
    cols = dim // CHUNKS
    groups = experts // GROUP
    me = lax.axis_index("tp")
    core, chip = lax.rem(me, 2), lax.div(me, 2)
    pair, far = me + 1 - 2 * core, me + 2 - 4 * chip
    pair_far = far + 1 - 2 * core

    def remote(src, dst, send, recv, to):
        return pltpu.make_async_remote_copy(src_ref=src, dst_ref=dst, send_sem=send, recv_sem=recv,
                                            device_id={"tp": to}, device_id_type=pl.DeviceIdType.MESH)

    def load_in(g):
        sl = pl.ds(g * GROUP, GROUP)
        return (pltpu.make_async_copy(w_gate.at[sl], w_in.at[sl, :, 0:part], wi_sem.at[0, g]),
                pltpu.make_async_copy(w_up.at[sl], w_in.at[sl, :, part:2 * part], wi_sem.at[1, g]))

    def load_down(g):
        sl = pl.ds(g * (w_dn.shape[0] // 4), w_dn.shape[0] // 4)
        return pltpu.make_async_copy(w_down.at[sl], w_dn.at[sl], wd_sem.at[g])

    barrier = pltpu.get_barrier_semaphore()
    for peer in (pair, far):
        pl.semaphore_signal(barrier, inc=1, device_id={"tp": peer}, device_id_type=pl.DeviceIdType.MESH)
    for g in range(groups):
        for copy in load_in(g):
            copy.start()
    pl.semaphore_wait(barrier, 2)

    def o_block(owner, h, kind, to):
        at = pl.ds(h * o_rows, o_rows)
        src = o_in.at[at] if kind < 2 else o_full.at[owner, at]
        return remote(src, o_full.at[owner, at], o_snd.at[kind, h], o_rcv.at[kind, h], to)

    sends = []

    def go(copy):
        copy.start()
        sends.append(copy)

    wo_copies = [remote(wo_own, wo_pair, wo_snd.at[0], wo_rcv.at[0], pair),
                 remote(wo_peer, wo_pair_far, wo_snd.at[1], wo_rcv.at[1], pair)]
    for h in range(2):
        go(o_block(me, h, 0, far))
    for h in range(2):
        go(o_block(me, h, 1, pair))
    for copy in wo_copies:
        go(copy)

    def relay_o(h):
        o_block(far, h, 0, far).wait_recv()
        go(o_block(far, h, 2, pair))

    def mid(h):
        o_block(pair, h, 1, pair).wait_recv()
        o_block(pair_far, h, 2, pair).wait_recv()
        at = pl.ds(h * o_rows, o_rows)
        total = hid[at, :].astype(jnp.float32)
        for part_o, part_w in ((o_in.at[at], wo_own), (o_full.at[far, at], wo_peer),
                               (o_full.at[pair, at], wo_pair), (o_full.at[pair_far, at], wo_pair_far)):
            total = total + jnp.dot(part_o[...], part_w[...], preferred_element_type=jnp.float32)
        x1[at, :] = total.astype(jnp.bfloat16)

    def routed(at, size):
        h2[at:at + size, :] = normed(x1[at:at + size, :].astype(jnp.float32), gain[...].astype(jnp.float32))
        logits = lax.dot_general(router[...], h2[at:at + size, :], (((1,), (1,)), ((), ())), preferred_element_type=jnp.float32)
        expert_id = lax.broadcasted_iota(jnp.int32, logits.shape, 0)
        picks = chosen[:, at:at + size]
        hit = expert_id == picks[0:1]
        for k in range(1, picks.shape[0]):
            hit = jnp.logical_or(hit, expert_id == picks[k:k + 1])
        shown = jnp.where(hit, logits, MASK_FILL)
        e = jnp.where(hit, jnp.exp(shown - jnp.max(shown, axis=0, keepdims=True)), 0.0)
        g = e / jnp.sum(e, axis=0, keepdims=True)
        gates[at:at + size, :] = jnp.concatenate([g, jnp.zeros((128 - experts, size), jnp.float32)], axis=0).T

    lane = lax.broadcasted_iota(jnp.int32, (block, 128), 1)

    def inner(p, unroll):
        def several(i, carry):
            if p == 0:
                for k in range(unroll // GROUP):
                    for copy in load_in(i * (unroll // GROUP) + k):
                        copy.wait()
            for k in range(unroll):
                e = i * unroll + k
                both = jnp.dot(h2[p * block:(p + 1) * block, :], w_in[e], preferred_element_type=jnp.float32)
                gate, up = both[:, :part], both[:, part:]
                weight = jnp.sum(jnp.where(lane == e, gates[p * block:(p + 1) * block, :], 0.0), axis=1, keepdims=True)
                act = weight * (gate / (1.0 + jnp.exp(-gate))) * up
                z[:, pl.ds(pl.multiple_of(e * part, part), part)] = act.astype(jnp.bfloat16)
            return carry
        lax.fori_loop(0, experts // unroll, several, 0)

    def down(p, c):
        acc[p, c] = jnp.dot(z[...], w_dn[:, c * cols:(c + 1) * cols], preferred_element_type=jnp.float32)
        go(pair_copy(p, c))

    def direct(p, c):
        return p * CHUNKS + c >= PARTS * CHUNKS - DIRECT

    def pair_copy(p, c):
        return remote(acc.at[p, c, pl.ds((1 - core) * (block // 2), block // 2)], from_pair.at[p, c], a_snd.at[p, c], a_rcv.at[p, c], pair)

    def far_copy(p, c):
        if direct(p, c):
            return remote(chip_sum.at[p, c], from_far.at[p, c], b_snd.at[p, c], b_rcv.at[p, c], far)
        size = block // 4
        return remote(chip_sum.at[p, c, pl.ds((1 - chip) * size, size)], from_far.at[p, c, 0:size], b_snd.at[p, c], b_rcv.at[p, c], far)

    def out_copy(p, c, kind, of_core, of_chip, to):
        if direct(p, c):
            at = pl.ds(p * block + of_core * (block // 2), block // 2)
        else:
            at = pl.ds(p * block + of_core * (block // 2) + of_chip * (block // 4), block // 4)
        ref = out.at[at, c * cols:(c + 1) * cols]
        return remote(ref, ref, c_snd.at[kind, p, c], c_rcv.at[kind, p, c], to)

    def stage_b(p, c):
        pair_copy(p, c).wait_recv()
        chip_sum[p, c] = acc[p, c, pl.ds(core * (block // 2), block // 2)] + from_pair[p, c]
        go(far_copy(p, c))

    def stage_c(p, c):
        far_copy(p, c).wait_recv()
        cut = slice(c * cols, (c + 1) * cols)
        base = p * block + core * (block // 2)
        if direct(p, c):
            at = pl.ds(base, block // 2)
            total = chip_sum[p, c] + from_far[p, c]
        else:
            at = pl.ds(base + chip * (block // 4), block // 4)
            total = chip_sum[p, c, pl.ds(chip * (block // 4), block // 4)] + from_far[p, c, 0:block // 4]
        out[at, cut] = (x1[at, cut].astype(jnp.float32) + total).astype(jnp.bfloat16)
        if not direct(p, c):
            go(out_copy(p, c, 0, core, chip, far))
        go(out_copy(p, c, 1, core, chip, pair))

    def stage_d(p, c):
        if not direct(p, c):
            out_copy(p, c, 0, core, 1 - chip, far).wait_recv()
            go(out_copy(p, c, 2, core, 1 - chip, pair))

    def stage_e(p, c):
        out_copy(p, c, 1, 1 - core, chip, pair).wait_recv()
        if not direct(p, c):
            out_copy(p, c, 2, 1 - core, 1 - chip, pair).wait_recv()

    relay_o(0)
    for g in range(4):
        load_down(g).start()
    for copy in wo_copies:
        copy.wait_recv()
    mid(0)
    if PARTS == 2:
        routed(0, block)
    relay_o(1)
    units = [(p, c) for p in range(PARTS) for c in range(CHUNKS)]
    if PARTS == 1:
        mid(1)
        routed(0, o_rows)
        routed(o_rows, o_rows)
        inner(0, 32)
        for g in range(4):
            load_down(g).wait()
        for c in range(CHUNKS):
            down(0, c)
            if c >= 2:
                stage_b(0, c - 2)
        for c in range(max(CHUNKS - 2, 0), CHUNKS):
            stage_b(0, c)
        rest = units
    else:
        inner(0, 32)
        for g in range(4):
            load_down(g).wait()
        for c in range(CHUNKS):
            down(0, c)
        mid(1)
        routed(block, block)
        for c in range(CHUNKS):
            stage_b(0, c)
        inner(1, 32)
        for c in range(CHUNKS):
            down(1, c)
            if c < CHUNKS - 1:
                stage_c(0, c)
        stage_b(1, 0)
        stage_c(0, CHUNKS - 1)
        for c in range(1, CHUNKS):
            stage_b(1, c)
        rest = [(1, c) for c in range(CHUNKS)]
        for c in range(CHUNKS):
            stage_d(0, c)
    for unit in rest:
        stage_c(*unit)
    for unit in rest:
        stage_d(*unit)
    for unit in units:
        stage_e(*unit)
    for copy in sends:
        copy.wait_send()


def expert_call(o, hidden_in, chosen_t, g_moe, router_t, w_o, wo_peer, w_gate, w_up, w_down):
    rows, dim = hidden_in.shape
    experts, _, part = w_gate.shape
    block, cols = rows // PARTS, dim // CHUNKS
    any_spec = pl.BlockSpec(memory_space=pltpu.HBM)
    vmem = pl.BlockSpec(memory_space=pltpu.VMEM)
    dma = pltpu.SemaphoreType.DMA
    bf, f32 = jnp.bfloat16, jnp.float32
    return pl.pallas_call(
        expert_kernel,
        out_shape=jax.ShapeDtypeStruct((rows, dim), bf),
        in_specs=[vmem] * 7 + [any_spec] * 3,
        out_specs=vmem,
        scratch_shapes=[
            pltpu.VMEM(w_o.shape, bf),
            pltpu.VMEM(w_o.shape, bf),
            pltpu.VMEM((4,) + o.shape, bf),
            pltpu.VMEM((experts, dim, 2 * part), bf),
            pltpu.VMEM((experts * part, dim), bf),
            pltpu.VMEM((rows, dim), bf),
            pltpu.VMEM((rows, dim), bf),
            pltpu.VMEM((rows, 128), f32),
            pltpu.VMEM((block, experts * part), bf),
            pltpu.VMEM((PARTS, CHUNKS, block, cols), f32),
            pltpu.VMEM((PARTS, CHUNKS, block // 2, cols), f32),
            pltpu.VMEM((PARTS, CHUNKS, block // 2, cols), f32),
            pltpu.VMEM((PARTS, CHUNKS, block // 2, cols), f32),
            dma((2, experts // GROUP)), dma((4,)), dma((2,)), dma((2,)), dma((3, 2)), dma((3, 2)),
            dma((PARTS, CHUNKS)), dma((PARTS, CHUNKS)), dma((PARTS, CHUNKS)), dma((PARTS, CHUNKS)),
            dma((3, PARTS, CHUNKS)), dma((3, PARTS, CHUNKS)),
        ],
        compiler_params=pltpu.CompilerParams(collective_id=0, has_side_effects=True, vmem_limit_bytes=40 << 20),
        cost_estimate=pl.CostEstimate(flops=7 * 10**9, bytes_accessed=28 * 10**6, transcendentals=0),
        name="experts",
    )(o, chosen_t, g_moe, router_t, hidden_in, w_o, wo_peer, *(pinned(w) for w in (w_gate, w_up, w_down.reshape(experts * part, dim))))


def solution(mesh):
    cache_spec = P("dp", None, "tp", None)
    in_specs = (P("dp", None), cache_spec, cache_spec, P("dp"), P("dp", None), P(None), P(None, "tp"), P(None, "tp"), P(None, "tp"), P("tp", None), P(None), P(None, None), P(None, None, "tp"), P(None, None, "tp"), P(None, "tp", None))
    out_specs = (P("dp", None), cache_spec, cache_spec)

    def layer_shard(hidden_in, k_cache, v_cache, seq_lens, chosen_experts, g_attn, w_q, w_k, w_v, w_o, g_moe, w_router, w_gate, w_up, w_down):
        rows, slots, kvh, hd = k_cache.shape
        as_t = lambda c: c.transpose(0, 2, 3, 1).reshape(rows, kvh * hd, slots)
        back = lambda c: c.reshape(rows, kvh, hd, slots).transpose(0, 3, 1, 2)
        wo_peer = lax.ppermute(w_o, "tp", [(0, 2), (1, 3), (2, 0), (3, 1)])
        o, k_n, v_n = attention_call(hidden_in, as_t(k_cache), as_t(v_cache), seq_lens, g_attn, w_q, w_k, w_v)
        hidden_out = expert_call(o, hidden_in, chosen_experts.T, g_moe, w_router.T, w_o, wo_peer, w_gate, w_up, w_down)
        return hidden_out, back(k_n), back(v_n)

    return jax.shard_map(layer_shard, mesh=mesh, in_specs=in_specs, out_specs=out_specs, check_vma=False)
```

```python
import math
import jax
import jax.numpy as jnp
from jax import lax
from jax.experimental import pallas as pl
from jax.experimental.pallas import tpu as pltpu
from jax.sharding import PartitionSpec as P

EPSILON = 1e-5
ROPE_THETA = 1000000.0
MASK_FILL = -1e30
BLOCK = 16
SLOTS = 8
AHEAD = 2
FIRST = 2
GROUP = 4
UNROLL = 16
PARTS = 2
CHUNKS = 2
DIRECT = 1


def pinned(array):
    return pltpu.with_memory_space_constraint(array, pltpu.HBM)


def normed(vector32, gain32):
    scale = lax.rsqrt(jnp.mean(vector32 * vector32, axis=-1, keepdims=True) + EPSILON)
    return (vector32 * scale * gain32).astype(jnp.bfloat16)


def attention_kernel(seq_lens, g_attn, hidden, w_q, w_k, w_v, k_in, v_in, o_out, k_out, v_out,
                     seq_s, seq_v, gain, hid, wqkv, kv_col, q_rows, o_rows, kbuf, vbuf, w_sem, k_rd, v_rd, k_wr, v_wr):
    rows, width, slots = k_in.shape
    heads_w = w_q.shape[1]
    half = width // 4
    steps = rows // BLOCK

    def read(i, slot):
        src = pl.ds(i * BLOCK, BLOCK)
        return (pltpu.make_async_copy(k_in.at[src], kbuf.at[slot], k_rd.at[slot]),
                pltpu.make_async_copy(v_in.at[src], vbuf.at[slot], v_rd.at[slot]))

    def write(i, slot):
        dst = pl.ds(i * BLOCK, BLOCK)
        return (pltpu.make_async_copy(kbuf.at[slot], k_out.at[dst], k_wr.at[slot]),
                pltpu.make_async_copy(vbuf.at[slot], v_out.at[dst], v_wr.at[slot]))

    loads = [pltpu.make_async_copy(hidden, hid, w_sem.at[0]),
             pltpu.make_async_copy(w_q, wqkv.at[:, 0:heads_w], w_sem.at[1]),
             pltpu.make_async_copy(w_k, wqkv.at[:, heads_w:heads_w + width], w_sem.at[2]),
             pltpu.make_async_copy(w_v, wqkv.at[:, heads_w + width:], w_sem.at[3]),
             pltpu.make_async_copy(seq_lens, seq_v, w_sem.at[4]),
             pltpu.make_async_copy(seq_lens, seq_s, w_sem.at[5]),
             pltpu.make_async_copy(g_attn, gain, w_sem.at[6])]
    for copy in loads:
        copy.start()
    for i in range(FIRST):
        for copy in read(i, i):
            copy.start()
    loads[4].wait()
    place = lax.broadcasted_iota(jnp.int32, (half, rows), 0).astype(jnp.float32)
    angles = jnp.exp(place * (-math.log(ROPE_THETA) / half)) * seq_v[...].astype(jnp.float32)[None, :]
    cos_t, sin_t = jnp.cos(angles), jnp.sin(angles)
    for copy in loads[:4] + loads[5:]:
        copy.wait()
    for i in range(FIRST, SLOTS):
        for copy in read(i, i):
            copy.start()
    h = normed(hid[...].astype(jnp.float32), gain[...].astype(jnp.float32))
    qkv_t = jnp.dot(h, wqkv[...], preferred_element_type=jnp.float32).T

    def rotated(at):
        a, c = qkv_t[at:at + half], qkv_t[at + half:at + 2 * half]
        return [a * cos_t - c * sin_t, c * cos_t + a * sin_t]

    k_t = jnp.concatenate(rotated(heads_w) + rotated(heads_w + 2 * half), axis=0)
    v_t = qkv_t[heads_w + width:]
    for part in range(rows // 128):
        lanes = slice(part * 128, part * 128 + 128)
        kv_col[part, 0:width] = k_t[:, lanes].astype(jnp.bfloat16)
        kv_col[part, width:] = v_t[:, lanes].astype(jnp.bfloat16)
    lane = lax.broadcasted_iota(jnp.int32, (rows, width), 1)
    for g in range(2):
        q_g = jnp.concatenate(rotated(g * 2 * half) + rotated((2 + g) * 2 * half), axis=0).T
        q_g = q_g.astype(jnp.bfloat16).astype(jnp.float32) * 0.125
        for kv in range(2):
            keep = (lane < 2 * half) if kv == 0 else (lane >= 2 * half)
            q_rows[pl.ds(kv * 2 + g, rows, stride=8), :] = jnp.where(keep, q_g, 0.0)
    for r in range(4, 8):
        q_rows[pl.ds(r, rows, stride=8), :] = jnp.zeros((rows, width), jnp.float32)

    slot_id = lax.broadcasted_iota(jnp.int32, (8, slots), 1)
    slot_bf = lax.broadcasted_iota(jnp.int32, (width, 128), 1).astype(jnp.float32).astype(jnp.bfloat16)

    row_id = lax.broadcasted_iota(jnp.int32, (128, 256), 0) - lax.div(lax.broadcasted_iota(jnp.int32, (128, 256), 1), 128)
    row_bf = row_id.astype(jnp.float32).astype(jnp.bfloat16)

    def step(i, carry):
        slot = lax.rem(i, SLOTS)
        for copy in read(i, slot):
            copy.wait()
        per = 128 // BLOCK
        columns = kv_col[lax.div(i, per)]
        first_row = lax.rem(i, per) * BLOCK
        cols = []
        for j in range(0, BLOCK, 2):
            pick = (row_bf == (first_row + j).astype(jnp.float32).astype(jnp.bfloat16))
            pick = jnp.where(pick, jnp.ones((), jnp.bfloat16), jnp.zeros((), jnp.bfloat16))
            both = jnp.dot(columns, pick, preferred_element_type=jnp.float32).astype(jnp.bfloat16)
            cols += [both[:, 0:128], both[:, 128:256]]
        places = [seq_s[i * BLOCK + j] for j in range(BLOCK)]

        def updated(buf, j, at):
            side = pl.ds(pl.multiple_of(lax.div(places[j], 128) * 128, 128), 128)
            here = slot_bf == lax.rem(places[j], 128).astype(jnp.float32).astype(jnp.bfloat16)
            buf[slot, j, :, side] = jnp.where(here, cols[j][at:at + width], buf[slot, j, :, side])
            return buf[slot, j]

        scores = []
        for j in range(BLOCK):
            q = q_rows[pl.ds((i * BLOCK + j) * 8, 8), :].astype(jnp.bfloat16)
            s = jnp.dot(q, updated(kbuf, j, 0), preferred_element_type=jnp.float32)
            scores.append(jnp.where(slot_id <= places[j], s, MASK_FILL))
        for j in range(BLOCK):
            s = scores[j]
            e = jnp.exp(s - jnp.max(s, axis=-1, keepdims=True))
            w = (e / jnp.sum(e, axis=-1, keepdims=True)).astype(jnp.bfloat16)
            o = lax.dot_general(w, updated(vbuf, j, width), (((1,), (1,)), ((), ())), preferred_element_type=jnp.float32)
            o_rows[pl.ds(j * 8, 8), :] = o
        for copy in write(i, slot):
            copy.start()
        low = lax.broadcasted_iota(jnp.int32, (BLOCK, width), 1) < 2 * half
        for kv in range(2):
            first = o_rows[pl.ds(2 * kv, BLOCK, stride=8), :]
            second = o_rows[pl.ds(2 * kv + 1, BLOCK, stride=8), :]
            if kv == 0:
                second = pltpu.roll(second, 2 * half, axis=1)
            else:
                first = pltpu.roll(first, 2 * half, axis=1)
            o_out[pl.ds(i * BLOCK, BLOCK), kv * width:(kv + 1) * width] = jnp.where(low, first, second).astype(jnp.bfloat16)

        @pl.when(jnp.logical_and(i >= AHEAD, i < steps - SLOTS + AHEAD))
        def _():
            old = lax.rem(i + SLOTS - AHEAD, SLOTS)
            for copy in write(i - AHEAD, old):
                copy.wait()
            for copy in read(i + SLOTS - AHEAD, old):
                copy.start()
        return carry

    lax.fori_loop(0, steps, step, 0)
    for i in range(steps - SLOTS, steps):
        for copy in write(i, i % SLOTS):
            copy.wait()


def attention_call(hidden_in, k_t, v_t, seq_lens, g_attn, w_q, w_k, w_v):
    rows, width, slots = k_t.shape
    any_spec = pl.BlockSpec(memory_space=pltpu.HBM)
    vmem = pl.BlockSpec(memory_space=pltpu.VMEM)
    cache = jax.ShapeDtypeStruct(k_t.shape, k_t.dtype)
    dma = pltpu.SemaphoreType.DMA
    return pl.pallas_call(
        attention_kernel,
        out_shape=(jax.ShapeDtypeStruct((rows, w_q.shape[1]), jnp.bfloat16), cache, cache),
        in_specs=[any_spec] * 8,
        out_specs=(vmem, any_spec, any_spec),
        scratch_shapes=[
            pltpu.SMEM(seq_lens.shape, jnp.int32),
            pltpu.VMEM(seq_lens.shape, jnp.int32),
            pltpu.VMEM(g_attn.shape, jnp.bfloat16),
            pltpu.VMEM(hidden_in.shape, jnp.bfloat16),
            pltpu.VMEM((hidden_in.shape[1], w_q.shape[1] + 2 * width), jnp.bfloat16),
            pltpu.VMEM((rows // 128, 2 * width, 128), jnp.bfloat16),
            pltpu.VMEM((rows * 8, width), jnp.float32),
            pltpu.VMEM((BLOCK * 8, width), jnp.float32),
            pltpu.VMEM((SLOTS, BLOCK, width, slots), jnp.bfloat16),
            pltpu.VMEM((SLOTS, BLOCK, width, slots), jnp.bfloat16),
            dma((7,)), dma((SLOTS,)), dma((SLOTS,)), dma((SLOTS,)), dma((SLOTS,)),
        ],
        compiler_params=pltpu.CompilerParams(vmem_limit_bytes=26 << 20),
        cost_estimate=pl.CostEstimate(flops=10**9, bytes_accessed=70 * 10**6, transcendentals=0),
        name="attention",
    )(*(pinned(a) for a in (seq_lens, g_attn, hidden_in, w_q, w_k, w_v, k_t, v_t)))


def expert_kernel(o_in, chosen, gain, router, hid, wo_own, wo_peer, w_gate, w_up, w_down, out,
                  wo_pair, wo_pair_far, o_full, begun, w_in, w_dn, x1, h2, gates, z, acc, from_pair, chip_sum, from_far,
                  wi_sem, wd_sem, wo_snd, wo_rcv, o_snd, o_rcv, a_snd, a_rcv, b_snd, b_rcv, c_snd, c_rcv):
    experts, dim, part = w_gate.shape
    rows = hid.shape[0]
    o_rows = rows // 2
    block = rows // PARTS
    cols = dim // CHUNKS
    groups = experts // GROUP
    me = lax.axis_index("tp")
    core, chip = lax.rem(me, 2), lax.div(me, 2)
    pair, far = me + 1 - 2 * core, me + 2 - 4 * chip
    pair_far = far + 1 - 2 * core

    def remote(src, dst, send, recv, to):
        return pltpu.make_async_remote_copy(src_ref=src, dst_ref=dst, send_sem=send, recv_sem=recv,
                                            device_id={"tp": to}, device_id_type=pl.DeviceIdType.MESH)

    def load_in(g):
        sl = pl.ds(g * GROUP, GROUP)
        return (pltpu.make_async_copy(w_gate.at[sl], w_in.at[sl, :, 0:part], wi_sem.at[0, g]),
                pltpu.make_async_copy(w_up.at[sl], w_in.at[sl, :, part:2 * part], wi_sem.at[1, g]))

    def load_down(g):
        sl = pl.ds(g * (w_dn.shape[0] // 4), w_dn.shape[0] // 4)
        return pltpu.make_async_copy(w_down.at[sl], w_dn.at[sl], wd_sem.at[g])

    barrier = pltpu.get_barrier_semaphore()
    for peer in (pair, far):
        pl.semaphore_signal(barrier, inc=1, device_id={"tp": peer}, device_id_type=pl.DeviceIdType.MESH)
    for g in range(groups):
        for copy in load_in(g):
            copy.start()
    pl.semaphore_wait(barrier, 2)

    def o_block(owner, h, kind, to):
        at = pl.ds(h * o_rows, o_rows)
        src = o_in.at[at] if kind < 2 else o_full.at[owner, at]
        return remote(src, o_full.at[owner, at], o_snd.at[kind, h], o_rcv.at[kind, h], to)

    sends = []

    def go(copy):
        copy.start()
        sends.append(copy)

    wo_copies = [remote(wo_own, wo_pair, wo_snd.at[0], wo_rcv.at[0], pair),
                 remote(wo_peer, wo_pair_far, wo_snd.at[1], wo_rcv.at[1], pair)]
    for h in range(2):
        go(o_block(me, h, 0, far))
    for h in range(2):
        go(o_block(me, h, 1, pair))
    for copy in wo_copies:
        go(copy)

    def relay_o(h):
        o_block(far, h, 0, far).wait_recv()
        go(o_block(far, h, 2, pair))

    def mid(h):
        o_block(pair, h, 1, pair).wait_recv()
        o_block(pair_far, h, 2, pair).wait_recv()
        at = pl.ds(h * o_rows, o_rows)
        for c in range(2):
            cut = slice(c * (dim // 2), (c + 1) * (dim // 2))
            total = begun[h, c]
            for owner, part_w in ((far, wo_peer), (pair, wo_pair), (pair_far, wo_pair_far)):
                total = total + jnp.dot(o_full[owner, at, :], part_w[:, cut], preferred_element_type=jnp.float32)
            x1[at, cut] = total.astype(jnp.bfloat16)

    def routed(at, size):
        h2[at:at + size, :] = normed(x1[at:at + size, :].astype(jnp.float32), gain[...].astype(jnp.float32))
        logits = lax.dot_general(router[...], h2[at:at + size, :], (((1,), (1,)), ((), ())), preferred_element_type=jnp.float32)
        expert_id = lax.broadcasted_iota(jnp.int32, logits.shape, 0)
        picks = chosen[:, at:at + size]
        hit = expert_id == picks[0:1]
        for k in range(1, picks.shape[0]):
            hit = jnp.logical_or(hit, expert_id == picks[k:k + 1])
        shown = jnp.where(hit, logits, MASK_FILL)
        e = jnp.where(hit, jnp.exp(shown - jnp.max(shown, axis=0, keepdims=True)), 0.0)
        g = e / jnp.sum(e, axis=0, keepdims=True)
        gates[at:at + size, :] = jnp.concatenate([g, jnp.zeros((128 - experts, size), jnp.float32)], axis=0).T

    lane = lax.broadcasted_iota(jnp.int32, (block, 128), 1)

    def inner(p, unroll):
        def several(i, carry):
            if p == 0:
                for k in range(unroll // GROUP):
                    for copy in load_in(i * (unroll // GROUP) + k):
                        copy.wait()
            for k in range(unroll):
                e = i * unroll + k
                both = jnp.dot(h2[p * block:(p + 1) * block, :], w_in[e], preferred_element_type=jnp.float32)
                gate, up = both[:, :part], both[:, part:]
                weight = jnp.sum(jnp.where(lane == e, gates[p * block:(p + 1) * block, :], 0.0), axis=1, keepdims=True)
                act = weight * (gate / (1.0 + jnp.exp(-gate))) * up
                z[:, pl.ds(pl.multiple_of(e * part, part), part)] = act.astype(jnp.bfloat16)
            return carry
        lax.fori_loop(0, experts // unroll, several, 0)

    def down(p, c):
        acc[p, c] = jnp.dot(z[...], w_dn[:, c * cols:(c + 1) * cols], preferred_element_type=jnp.float32)
        go(pair_copy(p, c))

    def direct(p, c):
        return p * CHUNKS + c >= PARTS * CHUNKS - DIRECT

    def pair_copy(p, c):
        return remote(acc.at[p, c, pl.ds((1 - core) * (block // 2), block // 2)], from_pair.at[p, c], a_snd.at[p, c], a_rcv.at[p, c], pair)

    def far_copy(p, c):
        if direct(p, c):
            return remote(chip_sum.at[p, c], from_far.at[p, c], b_snd.at[p, c], b_rcv.at[p, c], far)
        size = block // 4
        return remote(chip_sum.at[p, c, pl.ds((1 - chip) * size, size)], from_far.at[p, c, 0:size], b_snd.at[p, c], b_rcv.at[p, c], far)

    def out_copy(p, c, kind, of_core, of_chip, to):
        if direct(p, c):
            at = pl.ds(p * block + of_core * (block // 2), block // 2)
        else:
            at = pl.ds(p * block + of_core * (block // 2) + of_chip * (block // 4), block // 4)
        ref = out.at[at, c * cols:(c + 1) * cols]
        return remote(ref, ref, c_snd.at[kind, p, c], c_rcv.at[kind, p, c], to)

    def stage_b(p, c):
        pair_copy(p, c).wait_recv()
        chip_sum[p, c] = acc[p, c, pl.ds(core * (block // 2), block // 2)] + from_pair[p, c]
        go(far_copy(p, c))

    def stage_c(p, c):
        far_copy(p, c).wait_recv()
        cut = slice(c * cols, (c + 1) * cols)
        base = p * block + core * (block // 2)
        if direct(p, c):
            at = pl.ds(base, block // 2)
            total = chip_sum[p, c] + from_far[p, c]
        else:
            at = pl.ds(base + chip * (block // 4), block // 4)
            total = chip_sum[p, c, pl.ds(chip * (block // 4), block // 4)] + from_far[p, c, 0:block // 4]
        out[at, cut] = (x1[at, cut].astype(jnp.float32) + total).astype(jnp.bfloat16)
        if not direct(p, c):
            go(out_copy(p, c, 0, core, chip, far))
        go(out_copy(p, c, 1, core, chip, pair))

    def stage_d(p, c):
        if not direct(p, c):
            out_copy(p, c, 0, core, 1 - chip, far).wait_recv()
            go(out_copy(p, c, 2, core, 1 - chip, pair))

    def stage_e(p, c):
        out_copy(p, c, 1, 1 - core, chip, pair).wait_recv()
        if not direct(p, c):
            out_copy(p, c, 2, 1 - core, 1 - chip, pair).wait_recv()

    for h in range(2):
        at = pl.ds(h * o_rows, o_rows)
        for c in range(2):
            cut = slice(c * (dim // 2), (c + 1) * (dim // 2))
            begun[h, c] = hid[at, cut].astype(jnp.float32) + jnp.dot(o_in[at, :], wo_own[:, cut], preferred_element_type=jnp.float32)
    relay_o(0)
    for g in range(4):
        load_down(g).start()
    for copy in wo_copies:
        copy.wait_recv()
    mid(0)
    if PARTS == 2:
        routed(0, block)
    relay_o(1)
    units = [(p, c) for p in range(PARTS) for c in range(CHUNKS)]
    if PARTS == 1:
        mid(1)
        routed(0, o_rows)
        routed(o_rows, o_rows)
        inner(0, 32)
        for g in range(4):
            load_down(g).wait()
        for c in range(CHUNKS):
            down(0, c)
            if c >= 2:
                stage_b(0, c - 2)
        for c in range(max(CHUNKS - 2, 0), CHUNKS):
            stage_b(0, c)
        rest = units
    else:
        inner(0, 32)
        for g in range(4):
            load_down(g).wait()
        for c in range(CHUNKS):
            down(0, c)
        mid(1)
        routed(block, block)
        for c in range(CHUNKS):
            stage_b(0, c)
        inner(1, 32)
        for c in range(CHUNKS):
            down(1, c)
            if c < CHUNKS - 1:
                stage_c(0, c)
        stage_b(1, 0)
        stage_c(0, CHUNKS - 1)
        for c in range(1, CHUNKS):
            stage_b(1, c)
        rest = [(1, c) for c in range(CHUNKS)]
        for c in range(CHUNKS):
            stage_d(0, c)
    for unit in rest:
        stage_c(*unit)
    for unit in rest:
        stage_d(*unit)
    for unit in units:
        stage_e(*unit)
    for copy in sends:
        copy.wait_send()


def expert_call(o, hidden_in, chosen_t, g_moe, router_t, w_o, wo_peer, w_gate, w_up, w_down):
    rows, dim = hidden_in.shape
    experts, _, part = w_gate.shape
    block, cols = rows // PARTS, dim // CHUNKS
    any_spec = pl.BlockSpec(memory_space=pltpu.HBM)
    vmem = pl.BlockSpec(memory_space=pltpu.VMEM)
    dma = pltpu.SemaphoreType.DMA
    bf, f32 = jnp.bfloat16, jnp.float32
    return pl.pallas_call(
        expert_kernel,
        out_shape=jax.ShapeDtypeStruct((rows, dim), bf),
        in_specs=[vmem] * 7 + [any_spec] * 3,
        out_specs=vmem,
        scratch_shapes=[
            pltpu.VMEM(w_o.shape, bf),
            pltpu.VMEM(w_o.shape, bf),
            pltpu.VMEM((4,) + o.shape, bf),
            pltpu.VMEM((2, 2, rows // 2, dim // 2), f32),
            pltpu.VMEM((experts, dim, 2 * part), bf),
            pltpu.VMEM((experts * part, dim), bf),
            pltpu.VMEM((rows, dim), bf),
            pltpu.VMEM((rows, dim), bf),
            pltpu.VMEM((rows, 128), f32),
            pltpu.VMEM((block, experts * part), bf),
            pltpu.VMEM((PARTS, CHUNKS, block, cols), f32),
            pltpu.VMEM((PARTS, CHUNKS, block // 2, cols), f32),
            pltpu.VMEM((PARTS, CHUNKS, block // 2, cols), f32),
            pltpu.VMEM((PARTS, CHUNKS, block // 2, cols), f32),
            dma((2, experts // GROUP)), dma((4,)), dma((2,)), dma((2,)), dma((3, 2)), dma((3, 2)),
            dma((PARTS, CHUNKS)), dma((PARTS, CHUNKS)), dma((PARTS, CHUNKS)), dma((PARTS, CHUNKS)),
            dma((3, PARTS, CHUNKS)), dma((3, PARTS, CHUNKS)),
        ],
        compiler_params=pltpu.CompilerParams(collective_id=0, has_side_effects=True, vmem_limit_bytes=40 << 20),
        cost_estimate=pl.CostEstimate(flops=7 * 10**9, bytes_accessed=28 * 10**6, transcendentals=0),
        name="experts",
    )(o, chosen_t, g_moe, router_t, hidden_in, w_o, wo_peer, *(pinned(w) for w in (w_gate, w_up, w_down.reshape(experts * part, dim))))


def solution(mesh):
    cache_spec = P("dp", None, "tp", None)
    in_specs = (P("dp", None), cache_spec, cache_spec, P("dp"), P("dp", None), P(None), P(None, "tp"), P(None, "tp"), P(None, "tp"), P("tp", None), P(None), P(None, None), P(None, None, "tp"), P(None, None, "tp"), P(None, "tp", None))
    out_specs = (P("dp", None), cache_spec, cache_spec)

    def layer_shard(hidden_in, k_cache, v_cache, seq_lens, chosen_experts, g_attn, w_q, w_k, w_v, w_o, g_moe, w_router, w_gate, w_up, w_down):
        rows, slots, kvh, hd = k_cache.shape
        as_t = lambda c: c.transpose(0, 2, 3, 1).reshape(rows, kvh * hd, slots)
        back = lambda c: c.reshape(rows, kvh, hd, slots).transpose(0, 3, 1, 2)
        wo_peer = lax.ppermute(w_o, "tp", [(0, 2), (1, 3), (2, 0), (3, 1)])
        o, k_n, v_n = attention_call(hidden_in, as_t(k_cache), as_t(v_cache), seq_lens, g_attn, w_q, w_k, w_v)
        hidden_out = expert_call(o, hidden_in, chosen_experts.T, g_moe, w_router.T, w_o, wo_peer, w_gate, w_up, w_down)
        return hidden_out, back(k_n), back(v_n)

    return jax.shard_map(layer_shard, mesh=mesh, in_specs=in_specs, out_specs=out_specs, check_vma=False)
```
